128 devices in a mesh: band: 8 (over y, x_hi), slab: 16 (over x_lo, z, core).
Axes of the slice: x: 4 (x_hi: 2, x_lo: 2; x = x_hi * 2 + x_lo), y: 4, z: 4, core: 2. Of those that a mesh axis runs over, the one named last changes fastest.
Arguments:
- band_block: float32 [8, 2, 2, 128, 128, 128], P(None, None, None, 'band', 'slab'), may hold values from -24 to 24
- material_grid: int32 [128, 128, 128], P('slab'), may hold values from 0 to 3
- inverse_permittivity: float32 [4], replicated, may hold values from 0.077 to 1
- bloch_index: int32 [1], replicated, may hold values from 0 to 7
Outputs:
- search_block: float32 [8, 2, 2, 128, 128, 128], P(None, None, None, 'band', 'slab')
- correlation: float32 [2, 16, 16], replicated
- projected: float32 [2, 16, 16], replicated
The draws below stay inside these ranges and needn't reach their ends.
All inputs are finite; a program needn't handle non-finite values.
Results may differ from the reference program's by a relative error of at most 0.00005.
Values sent between devices are 32-bit elements; how exact they have to be, the bound alone decides.
A program may use at most 192 MiB of HBM per device.

```python
import math
import jax
import jax.numpy as jnp
from jax import lax

NX = 128
NY = 128
NZ = 128
MATERIALS = 4
KPOINTS = 8
BANDS = 8
NPTS = 2097152


def signed_fraction(length):
    indices = jnp.arange(length, dtype=jnp.int32)
    signed = jnp.where(indices >= length // 2, indices - length, indices).astype(jnp.float32)
    return signed / length


def draw_band_block(key, part):
    own_key = jax.random.fold_in(key, 11)
    common_key = jax.random.fold_in(key, 12)
    grid_shape = (BANDS, 2, 2, NZ, NY, NX)
    common = jnp.clip(jax.random.normal(common_key, (1, 2, 2, NZ, NY, NX), jnp.float32), -4.0, 4.0)
    own = jnp.clip(jax.random.normal(own_key, grid_shape, jnp.float32), -4.0, 4.0)
    depth_part = signed_fraction(NZ)[:, None, None]
    height_part = signed_fraction(NY)[None, :, None]
    width_part = signed_fraction(NX)[None, None, :]
    envelope = 3.0 / (1.0 + 12.0 * (depth_part * depth_part + height_part * height_part + width_part * width_part))
    return (envelope * (own + 0.7 * common)).astype(jnp.float32)


def set_ends(drawn, key, smallest, largest):
    index_at = [jax.random.randint(jax.random.fold_in(key, axis), (), 0, length) for axis, length in enumerate(drawn.shape)]
    longest = drawn.shape.index(max(drawn.shape))
    next_to = index_at[:longest] + [(index_at[longest] + 1) % drawn.shape[longest]] + index_at[longest + 1:]
    return drawn.at[tuple(index_at)].set(smallest).at[tuple(next_to)].set(largest)


def setup_inputs(seed: int = 0) -> dict:
    key_list = jax.random.split(jax.random.key(seed), 5)
    band_block = draw_band_block(jax.random.fold_in(key_list[4], 71), 0)
    material_grid = set_ends(jax.random.randint(key_list[1], (NZ, NY, NX), 0, MATERIALS), jax.random.fold_in(key_list[1], 1), 0, MATERIALS - 1).astype(jnp.int32)
    inverse_permittivity = jnp.clip(jnp.exp(jax.random.uniform(key_list[2], (MATERIALS,), jnp.float32, math.log(0.077), math.log(1.0))), 0.077, 1.0)
    bloch_index = jax.random.randint(key_list[3], (1,), 0, KPOINTS).astype(jnp.int32)
    return dict(band_block=band_block, material_grid=material_grid, inverse_permittivity=inverse_permittivity, bloch_index=bloch_index)


HIGHEST = lax.Precision.HIGHEST

def axis_values(length, weight, fraction, offset, extent):
    indices = offset + jnp.arange(extent, dtype=jnp.int32)
    signed = jnp.where(indices >= length // 2, indices - length, indices).astype(jnp.float32)
    return 2.0 * math.pi / length * (signed + weight * fraction)

def frame(depth_wave, height_wave, width_wave):
    depth_term = depth_wave[:, None, None]
    height_term = height_wave[None, :, None]
    width_term = width_wave[None, None, :]
    planar = jnp.sqrt(width_term * width_term + height_term * height_term)
    magnitude = jnp.sqrt(planar * planar + depth_term * depth_term)
    grid_shape = magnitude.shape
    primary = [jnp.broadcast_to(height_term / planar, grid_shape), jnp.broadcast_to(-width_term / planar, grid_shape), jnp.zeros(grid_shape, magnitude.dtype)]
    secondary = [width_term * depth_term / (magnitude * planar), height_term * depth_term / (magnitude * planar), jnp.broadcast_to(-planar / magnitude, grid_shape)]
    return (primary, secondary, magnitude)

def curl_field(block, primary, secondary, magnitude):
    first_comp = block[:, 0]
    second_comp = block[:, 1]
    parts = [magnitude * (first_comp * secondary[component] - second_comp * primary[component]) for component in range(3)]
    return jnp.stack(parts, axis=1).reshape((-1,) + first_comp.shape[1:])

def project_back(spectrum, primary, secondary, magnitude, band_count):
    grouped = spectrum.reshape((band_count, 3) + spectrum.shape[1:])
    along_second = grouped[:, 0] * secondary[0] + grouped[:, 1] * secondary[1] + grouped[:, 2] * secondary[2]
    along_primary = grouped[:, 0] * primary[0] + grouped[:, 1] * primary[1] + grouped[:, 2] * primary[2]
    return jnp.stack([magnitude * along_second, -magnitude * along_primary], axis=1)

def operate(block, inverse_cells, primary, secondary, magnitude):

    def one_band(single):
        curled = curl_field(single[None], primary, secondary, magnitude)
        spectrum = curled[:, 0] + 1j * curled[:, 1]
        spatial = jnp.fft.ifftn(spectrum, axes=(1, 2, 3)) * inverse_cells
        returned = jnp.fft.fftn(spatial, axes=(1, 2, 3))
        values = jnp.stack([jnp.real(returned), jnp.imag(returned)], axis=1)
        return project_back(values, primary, secondary, magnitude, 1)[0]
    return lax.map(one_band, block)

def gram_parts(left, right):
    left_real = left[:, :, 0].reshape(left.shape[0], -1)
    left_imag = left[:, :, 1].reshape(left.shape[0], -1)
    right_real = right[:, :, 0].reshape(right.shape[0], -1)
    right_imag = right[:, :, 1].reshape(right.shape[0], -1)
    inner_product = lambda first_rows, second_rows: jnp.einsum('km,jm->kj', first_rows, second_rows, precision=HIGHEST)
    real_sum = inner_product(left_real, right_real) + inner_product(left_imag, right_imag)
    imag_sum = inner_product(left_real, right_imag) - inner_product(left_imag, right_real)
    return (real_sum / NPTS, imag_sum / NPTS)

def reference(band_block, material_grid, inverse_permittivity, bloch_index):
    fraction = (bloch_index[0].astype(jnp.float32) + 1.0) / KPOINTS
    primary, secondary, magnitude = frame(axis_values(NZ, 0.2, fraction, 0, NZ), axis_values(NY, 0.35, fraction, 0, NY), axis_values(NX, 0.5, fraction, 0, NX))
    inverse_cells = inverse_permittivity[material_grid]
    image = operate(band_block, inverse_cells, primary, secondary, magnitude)
    correlation_real, correlation_imag = gram_parts(band_block, band_block)
    cross_real, cross_imag = gram_parts(band_block, image)
    system = jnp.concatenate([jnp.concatenate([correlation_real, -correlation_imag], 1), jnp.concatenate([correlation_imag, correlation_real], 1)], 0)
    right_side = jnp.concatenate([cross_real, cross_imag], 0)
    solution = jnp.linalg.solve(system, right_side)
    mixing_real = solution[:BANDS]
    mixing_imag = solution[BANDS:]
    block_real = band_block[:, :, 0]
    block_imag = band_block[:, :, 1]
    combine = lambda data, mixing: jnp.einsum('iabcd,ij->jabcd', data, mixing, precision=HIGHEST)
    residual_real = image[:, :, 0] - (combine(block_real, mixing_real) - combine(block_imag, mixing_imag))
    residual_imag = image[:, :, 1] - (combine(block_real, mixing_imag) + combine(block_imag, mixing_real))
    search_block = jnp.stack([residual_real, residual_imag], axis=2) / (magnitude * magnitude + 1.0)
    search_image = operate(search_block, inverse_cells, primary, secondary, magnitude)
    stacked = jnp.concatenate([band_block, search_block], 0)
    images = jnp.concatenate([image, search_image], 0)
    full_real, full_imag = gram_parts(stacked, stacked)
    proj_real, proj_imag = gram_parts(stacked, images)
    return (search_block, jnp.stack([full_real, full_imag], 0), jnp.stack([proj_real, proj_imag], 0))
```

```python
import functools
import math

import jax
import jax.numpy as jnp
import numpy as np
from jax import lax
from jax.experimental import pallas as pl
from jax.experimental.pallas import tpu as pltpu
from jax.sharding import Mesh
from jax.sharding import PartitionSpec as P

KPOINTS = 8
N = 128
CELLS = N * N * N
BANDS = 8
BAND = ("band_0", "band_1")
SLAB = ("slab_0", "slab_1", "slab_2")
HIGHEST = lax.Precision.HIGHEST
F32 = jnp.float32
BF16 = jnp.bfloat16


def _rot(angle):
    c, s = np.cos(angle), np.sin(angle)
    return np.stack([np.stack([c, -s]), np.stack([s, c])])


def _halves(table):
    high = table.astype(BF16)
    low = (table - high.astype(np.float64)).astype(BF16)
    return high, low


def _left(table):
    high, low = _halves(table)
    return np.concatenate([high, high, low], 1)


def _right(table):
    high, low = _halves(table)
    return np.concatenate([high, high, low], 0)


def tables():
    tau = 2.0 * math.pi
    i128, i16, i8 = np.arange(128), np.arange(16), np.arange(8)
    r = _rot(tau / 128 * (i128[:, None] * i128[None, :] % 128))
    ta = r.reshape(2, 2, 16, 8, 128).transpose(2, 0, 3, 1, 4).reshape(256, 256)
    r = _rot(tau / 8 * (i8[:, None] * i8[None, :] % 8))
    kz = np.einsum("abzs,xy->azxsby", r, np.eye(8)).reshape(128, 128)
    r = _rot(tau / 16 * (i16[:, None] * i16[None, :] % 16))
    wz = np.einsum("abos,xy->bsxaoy", r, np.eye(8)).reshape(256, 256)
    r = _rot(tau / 16 * (i16[:, None] * i16[None, :] % 16)).reshape(2, 2, 16, 2, 8)
    ky = np.einsum("abolq,xy->aoxqlby", r, np.eye(8)).reshape(256, 256)
    r = _rot(tau / 8 * (i8[:, None] * i8[None, :] % 8))
    wy = np.einsum("abos,xy->bxsayo", r, np.eye(16)).reshape(256, 256)
    lane = np.arange(128)
    az = tau / 128 * ((np.arange(64) // 8)[:, None] * (lane // 8)[None, :])
    ay = tau / 128 * ((np.arange(128) // 8)[:, None] * (lane % 8)[None, :])
    twz = np.stack([np.cos(az), np.sin(az)]).astype(np.float32)
    twy = np.stack([np.cos(ay), np.sin(ay)]).astype(np.float32)
    gather = np.zeros((128, 16), np.float32)
    for band in range(8):
        for part in range(2):
            gather[(band * 2 + part) * 8 : (band * 2 + part + 1) * 8, part * 8 + band] = 1.0
    turn = np.zeros((16, 16), np.float32)
    turn[:8, 8:] = np.eye(8)
    turn[8:, :8] = -np.eye(8)
    turned = gather @ turn.T
    collect = np.concatenate([gather.T, turned.T], 0)
    place = np.zeros((4, 2, 128, 128), np.float32)
    for slot in range(4):
        place[slot, 0, :, slot * 16 : slot * 16 + 16] = gather
        place[slot, 1, :, slot * 16 : slot * 16 + 16] = turned
    spread = np.zeros((128, 128), np.float32)
    spread[16:32] = gather.T
    same = (lane[:, None] % 8 == lane[None, :] % 8).astype(np.float32)
    return dict(
        ta=_left(ta), tat=_left(ta.T), kz=_left(kz), kzt=_left(kz.T), ky=_left(ky), kyt=_left(ky.T),
        wz=_right(wz), wzt=_right(wz.T), wy=_right(wy), wyt=_right(wy.T),
        twz=twz, twy=twy, collect=collect, place=place, spread=spread, gather=gather, same=same,
    )


NAMES = ("ta", "tat", "kz", "kzt", "ky", "kyt", "wz", "wzt", "wy", "wyt", "twz", "twy",
         "collect", "place", "spread", "gather", "same")


def parts(x):
    high = x.astype(BF16)
    low = (x - high.astype(F32)).astype(BF16)
    return high, low


def rows_dot(table3, x):
    high, low = parts(x)
    return jnp.dot(table3[...], jnp.concatenate([high, low, high], 0), preferred_element_type=F32)


def lanes_dot(x, table3):
    high, low = parts(x)
    return jnp.dot(jnp.concatenate([high, low, high], 1), table3[...], preferred_element_type=F32)


def exact_dot(x, y):
    return jnp.dot(x, y, precision=HIGHEST, preferred_element_type=F32)


def turn_by(re, im, cosine, sine):
    return re * cosine - im * sine, re * sine + im * cosine


def turn_back(re, im, cosine, sine):
    return re * cosine + im * sine, im * cosine - re * sine


def cut(x, size, axis=1):
    return [lax.slice_in_dim(x, k, k + size, axis=axis) for k in range(0, x.shape[axis], size)]


def z_forward(tab, blocks):
    mixed = rows_dot(tab["kz"], blocks)
    cosine, sine = tab["twz"][0], tab["twz"][1]
    pairs = [turn_by(b[:64], b[64:], cosine, sine) for b in cut(mixed, 128)]
    both = jnp.concatenate(
        [jnp.concatenate([a for a, _ in pairs], 0), jnp.concatenate([b for _, b in pairs], 0)], 1
    )
    return lanes_dot(both, tab["wz"])


def z_back(tab, both):
    mixed = lanes_dot(both, tab["wzt"])
    cosine, sine = tab["twz"][0], tab["twz"][1]
    blocks = []
    for b in cut(mixed, 64, 0):
        re, im = turn_back(b[:, :128], b[:, 128:], cosine, sine)
        blocks.append(jnp.concatenate([re, im], 0))
    return rows_dot(tab["kzt"], jnp.concatenate(blocks, 1))


def y_forward(tab, blocks):
    mixed = rows_dot(tab["ky"], blocks)
    cosine, sine = tab["twy"][0], tab["twy"][1]
    pairs = [turn_by(b[:128], b[128:], cosine, sine) for b in cut(mixed, 128)]
    both = jnp.concatenate(
        [jnp.concatenate([a for a, _ in pairs], 0), jnp.concatenate([b for _, b in pairs], 0)], 1
    )
    return lanes_dot(both, tab["wy"])


def y_back(tab, both):
    mixed = lanes_dot(both, tab["wyt"])
    cosine, sine = tab["twy"][0], tab["twy"][1]
    blocks = []
    for b in cut(mixed, 128, 0):
        re, im = turn_back(b[:, :128], b[:, 128:], cosine, sine)
        blocks.append(jnp.concatenate([re, im], 0))
    return rows_dot(tab["kyt"], jnp.concatenate(blocks, 1))


def axis_values(length, weight, fraction, indices):
    signed = jnp.where(indices >= length // 2, indices - length, indices).astype(F32)
    return 2.0 * math.pi / length * (signed + weight * fraction)


def kernel(bloch_ref, band_ref, cell_ref, *refs):
    tab = dict(zip(NAMES, refs[: len(NAMES)]))
    (out_ref, first_ref, second_ref, coef, xt, image, search, fields,
     s_a, r_a, s_b, r_b, s_c, r_c, s_d, r_d, s_small, r_one, r_two,
     send_x, recv_x, send_small, recv_small) = refs[len(NAMES):]
    y_me, xh_me, xl_me = (lax.axis_index(a) for a in ("band_0", "band_1", "slab_0"))
    z_me, c_me = lax.axis_index("slab_1"), lax.axis_index("slab_2")
    p_me = xl_me * 8 + y_me * 2 + xh_me
    q_me = z_me * 2 + c_me
    x_me = xh_me * 2 + xl_me

    def wide_peer(k):
        y = (y_me + k // 4) % 4
        x = (x_me + k % 4) % 4
        return {"band_0": y, "band_1": x // 2, "slab_0": x % 2}, (x % 2) * 8 + y * 2 + x // 2

    def deep_peer(k):
        z = (z_me + k // 2) % 4
        c = (c_me + k % 2) % 2
        return {"slab_1": z, "slab_2": c}, z * 2 + c

    barrier = pltpu.get_barrier_semaphore()
    for k in range(1, 16):
        pl.semaphore_signal(barrier, inc=1, device_id=wide_peer(k)[0], device_id_type=pl.DeviceIdType.MESH)
    for k in range(1, 8):
        pl.semaphore_signal(barrier, inc=1, device_id=deep_peer(k)[0], device_id_type=pl.DeviceIdType.MESH)
    pl.semaphore_wait(barrier, 22)

    def send(kind, t, source, target, peers, count, me):
        for k in range(1, count):
            device, slot = peers(k)
            pltpu.make_async_remote_copy(
                src_ref=source.at[slot], dst_ref=target.at[me],
                send_sem=send_x.at[kind, t], recv_sem=recv_x.at[kind, t],
                device_id=device, device_id_type=pl.DeviceIdType.MESH,
            ).start()
        target[me] = source[me]

    def descriptor(kind, t, source, target, count):
        return pltpu.make_async_remote_copy(
            src_ref=source.at[pl.ds(0, count - 1)], dst_ref=target.at[pl.ds(0, count - 1)],
            send_sem=send_x.at[kind, t], recv_sem=recv_x.at[kind, t],
            device_id=deep_peer(1)[0], device_id_type=pl.DeviceIdType.MESH,
        )

    def start_sum(slot):
        for k in range(1, 16):
            device, _ = wide_peer(k)
            pltpu.make_async_remote_copy(
                src_ref=s_small.at[slot, 0], dst_ref=r_one.at[slot, p_me],
                send_sem=send_small.at[slot, 0], recv_sem=recv_small.at[slot, 0],
                device_id=device, device_id_type=pl.DeviceIdType.MESH,
            ).start()
        r_one[slot, p_me] = s_small[slot, 0]

    def small_wait(slot, step, target, count):
        return pltpu.make_async_remote_copy(
            src_ref=target.at[slot, pl.ds(0, count - 1)], dst_ref=target.at[slot, pl.ds(0, count - 1)],
            send_sem=send_small.at[slot, step], recv_sem=recv_small.at[slot, step],
            device_id=deep_peer(1)[0], device_id_type=pl.DeviceIdType.MESH,
        )

    def middle_sum(slot):
        small_wait(slot, 0, r_one, 16).wait_recv()
        s_small[slot, 1] = jnp.sum(r_one[slot], axis=0)
        for k in range(1, 8):
            device, _ = deep_peer(k)
            pltpu.make_async_remote_copy(
                src_ref=s_small.at[slot, 1], dst_ref=r_two.at[slot, q_me],
                send_sem=send_small.at[slot, 1], recv_sem=recv_small.at[slot, 1],
                device_id=device, device_id_type=pl.DeviceIdType.MESH,
            ).start()
        r_two[slot, q_me] = s_small[slot, 1]

    def finish_sum(slot):
        small_wait(slot, 1, r_two, 8).wait_recv()
        return jnp.sum(r_two[slot], axis=0)

    fraction = (bloch_ref[0].astype(F32) + 1.0) / KPOINTS
    row = lax.broadcasted_iota(jnp.int32, (N, N), 0)
    lane = lax.broadcasted_iota(jnp.int32, (N, N), 1)
    qx = axis_values(N, 0.5, fraction, row)
    qz = axis_values(N, 0.2, fraction, (y_me * 2 + xh_me) * 16 + lane // 8)
    qy = axis_values(N, 0.35, fraction, (xl_me * 8 + q_me) * 8 + lane % 8)
    planar = jnp.sqrt(qx * qx + qy * qy)
    magnitude = jnp.sqrt(planar * planar + qz * qz)
    coef[0] = magnitude * (qx * qz / (magnitude * planar))
    coef[1] = magnitude * (qy * qz / (magnitude * planar))
    coef[2] = magnitude * (-planar / magnitude)
    coef[3] = magnitude * (qy / planar)
    coef[4] = magnitude * (-qx / planar)
    coef[5] = 1.0 / (magnitude * magnitude + 1.0)

    def curl_and_send(kind, t, block):
        columns = []
        for c in range(3):
            halves = []
            for part in range(2):
                term = coef[c] * block[part]
                if c < 2:
                    term = term - coef[3 + c] * block[2 + part]
                halves.append(term)
            columns.append(jnp.concatenate(halves, 0))
        spread_x = rows_dot(tab["ta"][...], jnp.concatenate(columns, 1))
        for c in range(3):
            s_a[kind // 4, t, :, c] = spread_x[:, c * N : (c + 1) * N].reshape(16, 2, 8, N)
        send(kind, t, s_a.at[kind // 4, t], r_a.at[kind // 4, t], wide_peer, 16, p_me)

    def z_stage(kind, t):
        op = kind // 4
        descriptor(kind - 1, t, s_a.at[op, t], r_a.at[op, t], 16).wait_recv()
        blocks = [r_a[op, t, pl.ds(xlo * 8, 8), c].reshape(N, N) for c in range(3) for xlo in range(2)]
        both = z_forward(tab, jnp.concatenate(blocks, 1))
        for k in range(6):
            for part in range(2):
                s_b[op, t, :, k, part] = both[k * 64 : (k + 1) * 64, part * N : (part + 1) * N].reshape(8, 8, N)
        send(kind, t, s_b.at[op, t], r_b.at[op, t], deep_peer, 8, q_me)

    def y_stage(kind, t):
        op = kind // 4
        descriptor(kind, t, s_b.at[op, t], r_b.at[op, t], 8).wait_recv()
        blocks = [r_b[op, t, :, pl.ds(2 * c, 2)].reshape(256, N) for c in range(3)]
        both = y_forward(tab, jnp.concatenate(blocks, 1))
        for c in range(3):
            for part in range(2):
                fields[t, c, part] = both[c * N : (c + 1) * N, part * N : (part + 1) * N].reshape(16, 8, N)
        return both

    def first_y_stage(t):
        both = y_stage(1, t)
        cell = cell_ref[...]
        cell = jnp.concatenate([jnp.concatenate([cell, cell], 1)] * 3, 0)
        back = y_back(tab, both * cell)
        for c in range(3):
            s_c[t, :, pl.ds(2 * c, 2)] = back[:, c * N : (c + 1) * N].reshape(8, 2, 2, 8, N)
        send(2, t, s_c.at[t], r_c.at[t], deep_peer, 8, q_me)

    def z_back_stage(t):
        descriptor(2, t, s_c.at[t], r_c.at[t], 8).wait_recv()
        rows = [
            jnp.concatenate([r_c[t, :, k, part].reshape(64, N) for part in range(2)], 1) for k in range(6)
        ]
        back = z_back(tab, jnp.concatenate(rows, 0))
        for c in range(3):
            for xlo in range(2):
                k = 2 * c + xlo
                s_d[t, pl.ds(xlo * 8, 8), c] = back[:, k * N : (k + 1) * N].reshape(8, 2, 8, N)
        send(3, t, s_d.at[t], r_d.at[t], wide_peer, 16, p_me)

    def x_back_stage(t):
        descriptor(3, t, s_d.at[t], r_d.at[t], 16).wait_recv()
        columns = [r_d[t, :, c].reshape(256, N) for c in range(3)]
        back = rows_dot(tab["tat"][...], jnp.concatenate(columns, 1))
        for part in range(2):
            g = [back[part * N : (part + 1) * N, c * N : (c + 1) * N] for c in range(3)]
            image[t, 0, part] = (g[0] * coef[0] + g[1] * coef[1] + g[2] * coef[2]).reshape(16, 8, N)
            image[t, 1, part] = (-(g[0] * coef[3] + g[1] * coef[4])).reshape(16, 8, N)

    def gram(left, right, groups, slot, scale=None):
        def body(g, total):
            comp, m0 = g // 2, (g % 2) * 8
            left_cols = [left[:, comp, :, m0 + m].reshape(N, N) for m in range(8)]
            if scale is None:
                right_cols = left_cols if right is left else [
                    right[:, comp, :, m0 + m].reshape(N, N) for m in range(8)
                ]
            else:
                right_cols = []
                for m in range(8):
                    weight = scale[pl.ds(pl.multiple_of((m0 + m) * 8, 8), 8), :]
                    right_cols.append((right[:, comp, :, m0 + m] * weight[None, None]).reshape(N, N))
            lh, ll = parts(jnp.concatenate(left_cols, 1))
            rh, rl = parts(jnp.concatenate(right_cols, 1))
            return total + lax.dot_general(
                jnp.concatenate([lh, ll, lh], 1), jnp.concatenate([rh, rh, rl], 1),
                (((1,), (1,)), ((), ())), preferred_element_type=F32,
            )
        total = lax.fori_loop(0, groups, body, jnp.zeros((N, N), F32))
        folded = exact_dot(tab["collect"][...], total * tab["same"][...])
        return exact_dot(folded[:16], tab["place"][slot, 0]) + exact_dot(folded[16:], tab["place"][slot, 1])

    def first_step(t, carry):
        @pl.when(t < 8)
        def _():
            for comp in range(2):
                for part in range(2):
                    xt[t, comp, part] = band_ref[t, comp, part].reshape(N, N).T.reshape(16, 8, N)
            curl_and_send(0, t, [xt[t, c, r].reshape(N, N) for c in range(2) for r in range(2)])

        @pl.when((t >= 1) & (t < 9))
        def _():
            z_stage(1, t - 1)

        @pl.when((t >= 2) & (t < 10))
        def _():
            first_y_stage(t - 2)

        @pl.when((t >= 3) & (t < 11))
        def _():
            z_back_stage(t - 3)

        @pl.when((t >= 4) & (t < 12))
        def _():
            x_back_stage(t - 4)

        @pl.when(t == 9)
        def _():
            s_small[0, 0] = gram(xt, xt, 4, 0) + gram(fields, fields, 6, 1, cell_ref)
            start_sum(0)

        @pl.when(t == 10)
        def _():
            middle_sum(0)

        return carry

    lax.fori_loop(0, 12, first_step, 0)

    system = finish_sum(0)
    first_ref[...] = system
    rows16 = lax.broadcasted_iota(jnp.int32, (16, N), 0)
    for k in range(16):
        pivot = system[k : k + 1] / system[k : k + 1, k : k + 1]
        system = jnp.where(rows16 == k, pivot, system - system[:, k : k + 1] * pivot)
    wide = exact_dot(system, tab["spread"][...])
    mixing = exact_dot(tab["gather"][...], wide).T * tab["same"][...]
    mix_high, mix_low = parts(mixing)
    mixing = jnp.concatenate([mix_high, mix_high, mix_low], 1)

    def residual_step(g, carry):
        comp, m0 = g // 2, (g % 2) * 8
        columns = jnp.concatenate([xt[:, comp, :, m0 + m].reshape(N, N) for m in range(8)], 1)
        mixed = rows_dot(mixing, columns)
        for m in range(8):
            scale = coef[5, pl.ds(pl.multiple_of((m0 + m) * 8, 8), 8), :]
            search[:, comp, :, m0 + m] = (
                image[:, comp, :, m0 + m] - mixed[:, m * N : (m + 1) * N].reshape(8, 2, 8, N)
            ) * scale[None, None]
        return carry

    lax.fori_loop(0, 4, residual_step, 0)

    def second_step(t, carry):
        @pl.when(t < 8)
        def _():
            curl_and_send(4, t, [search[t, c, r].reshape(N, N) for c in range(2) for r in range(2)])
            for comp in range(2):
                for part in range(2):
                    out_ref[t, comp, part] = search[t, comp, part].reshape(N, N).T.reshape(16, 8, N)

        @pl.when((t >= 1) & (t < 9))
        def _():
            z_stage(5, t - 1)

        @pl.when((t >= 2) & (t < 10))
        def _():
            y_stage(5, t - 2)

        @pl.when(t == 8)
        def _():
            s_small[1, 0] = gram(xt, search, 4, 0) + gram(search, search, 4, 1) + gram(search, image, 4, 2)

        return carry

    lax.fori_loop(0, 10, second_step, 0)
    s_small[1, 0] = s_small[1, 0] + gram(fields, fields, 6, 3, cell_ref)
    start_sum(1)
    middle_sum(1)
    second_ref[...] = finish_sum(1)

    def drain(t, carry):
        descriptor(0, t, s_a.at[0, t], r_a.at[0, t], 16).wait_send()
        descriptor(1, t, s_b.at[0, t], r_b.at[0, t], 8).wait_send()
        descriptor(2, t, s_c.at[t], r_c.at[t], 8).wait_send()
        descriptor(3, t, s_d.at[t], r_d.at[t], 16).wait_send()
        descriptor(4, t, s_a.at[1, t], r_a.at[1, t], 16).wait_send()
        descriptor(5, t, s_b.at[1, t], r_b.at[1, t], 8).wait_send()
        return carry

    lax.fori_loop(0, 8, drain, 0)
    for slot in range(2):
        small_wait(slot, 0, r_one, 16).wait_send()
        small_wait(slot, 1, r_two, 8).wait_send()


def shards(band_block, material_grid, inverse_permittivity, bloch_index):
    cells = jnp.zeros(material_grid.shape, F32)
    for material in range(inverse_permittivity.shape[0]):
        cells = cells + jnp.where(material_grid == material, inverse_permittivity[material], 0.0)
    cells = cells / CELLS
    block = lax.axis_index(BAND)
    cells = cells.reshape(8, N, 2, 8, 8)
    cells = lax.dynamic_index_in_dim(cells, block, 3, keepdims=False)
    cells = cells.transpose(2, 0, 1, 3).reshape(16, N, 8)
    cells = lax.all_to_all(cells, SLAB, split_axis=0, concat_axis=0, tiled=True)
    cells = cells.reshape(16, 8, 16, 8).transpose(2, 3, 0, 1).reshape(N, N)

    table = tables()
    vmem = pl.BlockSpec(memory_space=pltpu.VMEM)
    search, first, second = pl.pallas_call(
        kernel,
        out_shape=(
            jax.ShapeDtypeStruct(band_block.shape, F32),
            jax.ShapeDtypeStruct((16, N), F32),
            jax.ShapeDtypeStruct((16, N), F32),
        ),
        in_specs=[pl.BlockSpec(memory_space=pltpu.SMEM)] + [vmem] * (2 + len(NAMES)),
        out_specs=(vmem, vmem, vmem),
        scratch_shapes=[
            pltpu.VMEM((6, N, N), F32),
            pltpu.VMEM((8, 2, 2, 16, 8, N), F32),
            pltpu.VMEM((8, 2, 2, 16, 8, N), F32),
            pltpu.VMEM((8, 2, 2, 16, 8, N), F32),
            pltpu.VMEM((8, 3, 2, 16, 8, N), F32),
            pltpu.VMEM((2, 8, 16, 3, 2, 8, N), F32),
            pltpu.VMEM((2, 8, 16, 3, 2, 8, N), F32),
            pltpu.VMEM((2, 8, 8, 6, 2, 8, N), F32),
            pltpu.VMEM((2, 8, 8, 6, 2, 8, N), F32),
            pltpu.VMEM((8, 8, 6, 2, 8, N), F32),
            pltpu.VMEM((8, 8, 6, 2, 8, N), F32),
            pltpu.VMEM((8, 16, 3, 2, 8, N), F32),
            pltpu.VMEM((8, 16, 3, 2, 8, N), F32),
            pltpu.VMEM((2, 2, 16, N), F32),
            pltpu.VMEM((2, 16, 16, N), F32),
            pltpu.VMEM((2, 8, 16, N), F32),
            pltpu.SemaphoreType.DMA((6, 8)),
            pltpu.SemaphoreType.DMA((6, 8)),
            pltpu.SemaphoreType.DMA((2, 2)),
            pltpu.SemaphoreType.DMA((2, 2)),
        ],
        compiler_params=pltpu.CompilerParams(
            collective_id=0, has_side_effects=True, vmem_limit_bytes=63 * 1024 * 1024
        ),
    )(bloch_index, band_block, cells, *[jnp.asarray(table[name]) for name in NAMES])

    first = first / CELLS
    second = second / CELLS

    def pair(tile, slot):
        return tile[:8, slot * 16 : slot * 16 + 8], tile[:8, slot * 16 + 8 : slot * 16 + 16]

    def joined(corner, right, below, last):
        return jnp.concatenate(
            [jnp.concatenate([corner, right], 1), jnp.concatenate([below, last], 1)], 0
        )

    s_re, s_im = pair(first, 0)
    h_re, h_im = pair(first, 1)
    xs_re, xs_im = pair(second, 0)
    ss_re, ss_im = pair(second, 1)
    b_re, b_im = pair(second, 2)
    p_re, p_im = pair(second, 3)
    correlation = jnp.stack([joined(s_re, xs_re, xs_re.T, ss_re), joined(s_im, xs_im, -xs_im.T, ss_im)])
    projected = jnp.stack([joined(h_re, b_re.T, b_re, p_re), joined(h_im, -b_im.T, b_im, p_im)])
    return search, correlation, projected


def solution(mesh):
    finer = Mesh(
        mesh.devices.reshape(4, 2, 2, 4, 2), ("band_0", "band_1", "slab_0", "slab_1", "slab_2")
    )
    placed = (P(None, None, None, BAND, SLAB, None), P(SLAB, None, None), P(), P())
    return jax.shard_map(
        shards,
        mesh=finer,
        in_specs=placed,
        out_specs=(P(None, None, None, BAND, SLAB, None), P(), P()),
        check_vma=False,
    )
```

```python
import functools
import math

import jax
import jax.numpy as jnp
import numpy as np
from jax import lax
from jax.experimental import pallas as pl
from jax.experimental.pallas import tpu as pltpu
from jax.sharding import Mesh
from jax.sharding import PartitionSpec as P

KPOINTS = 8
N = 128
CELLS = N * N * N
BANDS = 8
BAND = ("band_0", "band_1")
SLAB = ("slab_0", "slab_1", "slab_2")
HIGHEST = lax.Precision.HIGHEST
F32 = jnp.float32
BF16 = jnp.bfloat16


def _rot(angle):
    c, s = np.cos(angle), np.sin(angle)
    return np.stack([np.stack([c, -s]), np.stack([s, c])])


def _halves(table):
    high = table.astype(BF16)
    low = (table - high.astype(np.float64)).astype(BF16)
    return high, low


def _left(table):
    high, low = _halves(table)
    return np.concatenate([high, low], 1)


def _right(table):
    high, low = _halves(table)
    return np.concatenate([high, low], 0)


def tables():
    tau = 2.0 * math.pi
    i128, i16, i8 = np.arange(128), np.arange(16), np.arange(8)
    r = _rot(tau / 128 * (i128[:, None] * i128[None, :] % 128))
    ta = r.reshape(2, 2, 16, 8, 128).transpose(2, 0, 3, 1, 4).reshape(256, 256)
    r = _rot(tau / 8 * (i8[:, None] * i8[None, :] % 8))
    kz = np.einsum("abzs,xy->azxsby", r, np.eye(8)).reshape(128, 128)
    r = _rot(tau / 16 * (i16[:, None] * i16[None, :] % 16))
    wz = np.einsum("abos,xy->bsxaoy", r, np.eye(8)).reshape(256, 256)
    r = _rot(tau / 16 * (i16[:, None] * i16[None, :] % 16)).reshape(2, 2, 16, 2, 8)
    ky = np.einsum("abolq,xy->aoxqlby", r, np.eye(8)).reshape(256, 256)
    r = _rot(tau / 8 * (i8[:, None] * i8[None, :] % 8))
    wy = np.einsum("abos,xy->bxsayo", r, np.eye(16)).reshape(256, 256)
    lane = np.arange(128)
    az = tau / 128 * ((np.arange(64) // 8)[:, None] * (lane // 8)[None, :])
    ay = tau / 128 * ((np.arange(128) // 8)[:, None] * (lane % 8)[None, :])
    twz = np.stack([np.cos(az), np.sin(az)]).astype(np.float32)
    twy = np.stack([np.cos(ay), np.sin(ay)]).astype(np.float32)
    gather = np.zeros((128, 16), np.float32)
    for band in range(8):
        for part in range(2):
            gather[(band * 2 + part) * 8 : (band * 2 + part + 1) * 8, part * 8 + band] = 1.0
    turn = np.zeros((16, 16), np.float32)
    turn[:8, 8:] = np.eye(8)
    turn[8:, :8] = -np.eye(8)
    turned = gather @ turn.T
    collect = np.concatenate([gather.T, turned.T], 0)
    place = np.zeros((2, 128, 128), np.float32)
    place[0, :, :16] = gather
    place[1, :, :16] = turned
    spread = np.zeros((128, 128), np.float32)
    spread[16:32] = gather.T
    order = np.zeros((128, 128), np.float32)
    order[lane, lane % 16 * 8 + lane // 16] = 1.0
    return dict(
        ta=_left(ta), tat=_left(ta.T), kz=_left(kz), kzt=_left(kz.T), ky=_left(ky), kyt=_left(ky.T),
        wz=_right(wz), wzt=_right(wz.T), wy=_right(wy), wyt=_right(wy.T),
        twz=twz, twy=twy, collect=collect, place=place, spread=spread, gather=gather, order=order.astype(BF16),
    )


NAMES = ("ta", "tat", "kz", "kzt", "ky", "kyt", "wz", "wzt", "wy", "wyt", "twz", "twy",
         "collect", "place", "spread", "gather", "order")


def parts(x):
    high = x.astype(BF16)
    low = (x - high.astype(F32)).astype(BF16)
    return high, low


def rows_dot(table, x):
    high, low = parts(x)
    k = x.shape[0]
    return jnp.dot(
        jnp.concatenate([table[:, :k], table[:, :k], table[:, k:]], 1),
        jnp.concatenate([high, low, high], 0),
        preferred_element_type=F32,
    )


def lanes_dot(x, table):
    high, low = parts(x)
    k = x.shape[1]
    return jnp.dot(
        jnp.concatenate([high, low, high], 1),
        jnp.concatenate([table[:k], table[:k], table[k:]], 0),
        preferred_element_type=F32,
    )


def exact_dot(x, y):
    return jnp.dot(x, y, precision=HIGHEST, preferred_element_type=F32)


def turn_by(re, im, cosine, sine):
    return re * cosine - im * sine, re * sine + im * cosine


def turn_back(re, im, cosine, sine):
    return re * cosine + im * sine, im * cosine - re * sine


def cut(x, size, axis=1):
    return [lax.slice_in_dim(x, k, k + size, axis=axis) for k in range(0, x.shape[axis], size)]


def z_forward(tab, blocks):
    mixed = rows_dot(tab["kz"], blocks)
    cosine, sine = tab["twz"][0], tab["twz"][1]
    pairs = [turn_by(b[:64], b[64:], cosine, sine) for b in cut(mixed, 128)]
    both = jnp.concatenate(
        [jnp.concatenate([a for a, _ in pairs], 0), jnp.concatenate([b for _, b in pairs], 0)], 1
    )
    return lanes_dot(both, tab["wz"])


def z_back(tab, both):
    mixed = lanes_dot(both, tab["wzt"])
    cosine, sine = tab["twz"][0], tab["twz"][1]
    blocks = []
    for b in cut(mixed, 64, 0):
        re, im = turn_back(b[:, :128], b[:, 128:], cosine, sine)
        blocks.append(jnp.concatenate([re, im], 0))
    return rows_dot(tab["kzt"], jnp.concatenate(blocks, 1))


def y_forward(tab, blocks):
    mixed = rows_dot(tab["ky"], blocks)
    cosine, sine = tab["twy"][0], tab["twy"][1]
    pairs = [turn_by(b[:128], b[128:], cosine, sine) for b in cut(mixed, 128)]
    both = jnp.concatenate(
        [jnp.concatenate([a for a, _ in pairs], 0), jnp.concatenate([b for _, b in pairs], 0)], 1
    )
    return lanes_dot(both, tab["wy"])


def y_back(tab, both):
    mixed = lanes_dot(both, tab["wyt"])
    cosine, sine = tab["twy"][0], tab["twy"][1]
    blocks = []
    for b in cut(mixed, 128, 0):
        re, im = turn_back(b[:, :128], b[:, 128:], cosine, sine)
        blocks.append(jnp.concatenate([re, im], 0))
    return rows_dot(tab["kyt"], jnp.concatenate(blocks, 1))


def axis_values(length, weight, fraction, indices):
    signed = jnp.where(indices >= length // 2, indices - length, indices).astype(F32)
    return 2.0 * math.pi / length * (signed + weight * fraction)


LAG_BACK = 7
LAG_NEXT = 11
MESH_ID = pl.DeviceIdType.MESH


def kernel(bloch_ref, weight_ref, band_hbm, material_hbm, *refs):
    count = len(NAMES)
    table_hbm = refs[:count]
    (out_hbm, corr_ref, proj_ref, coef, band_in, material, cell, xt, image, search, out_stage, fields,
     s_a, r_a, s_b, r_b, s_c, r_c, s_d, r_d, s_cell, r_cell, s_small, r_one, r_two, first_sum, mixing,
     send_x, recv_x, send_small, recv_small, cell_sem, in_sem, table_sem, out_sem) = refs[count : -count]
    tab = dict(zip(NAMES, refs[-count:]))
    y_me, xh_me, xl_me = (lax.axis_index(a) for a in ("band_0", "band_1", "slab_0"))
    z_me, c_me = lax.axis_index("slab_1"), lax.axis_index("slab_2")
    zb_me = y_me * 2 + xh_me
    p_me = xl_me * 8 + zb_me
    q_me = z_me * 2 + c_me
    x_me = xh_me * 2 + xl_me

    def wide_peer(k):
        y = (y_me + k // 4) % 4
        x = (x_me + k % 4) % 4
        return {"band_0": y, "band_1": x // 2, "slab_0": x % 2}, (x % 2) * 8 + y * 2 + x // 2

    def deep_peer(k):
        z = (z_me + k // 2) % 4
        c = (c_me + k % 2) % 2
        return {"slab_1": z, "slab_2": c}, z * 2 + c

    def slab_peer(k):
        xl = (xl_me + k // 8) % 2
        z = (z_me + k // 2 % 4) % 4
        c = (c_me + k % 2) % 2
        return {"slab_0": xl, "slab_1": z, "slab_2": c}, xl, z * 2 + c

    def band_copy(t):
        return pltpu.make_async_copy(band_hbm.at[t], band_in.at[t], in_sem.at[t])

    def table_copy(k):
        return pltpu.make_async_copy(table_hbm[k], tab[NAMES[k]], table_sem.at[k])

    material_copy = pltpu.make_async_copy(material_hbm, material, cell_sem.at[2])
    band_copy(0).start()
    table_copy(0).start()
    for t in range(1, 8):
        band_copy(t).start()
    for k in range(1, count):
        table_copy(k).start()
    material_copy.start()

    barrier = pltpu.get_barrier_semaphore()
    for k in range(1, 16):
        pl.semaphore_signal(barrier, inc=1, device_id=wide_peer(k)[0], device_id_type=MESH_ID)
    for k in range(1, 8):
        pl.semaphore_signal(barrier, inc=1, device_id=deep_peer(k)[0], device_id_type=MESH_ID)
    for k in range(9, 16):
        pl.semaphore_signal(barrier, inc=1, device_id=slab_peer(k)[0], device_id_type=MESH_ID)

    fraction = (bloch_ref[0].astype(F32) + 1.0) / KPOINTS
    row = lax.broadcasted_iota(jnp.int32, (N, N), 0)
    lane = lax.broadcasted_iota(jnp.int32, (N, N), 1)
    qx = axis_values(N, 0.5, fraction, row)
    qz = axis_values(N, 0.2, fraction, zb_me * 16 + lane // 8)
    qy = axis_values(N, 0.35, fraction, (xl_me * 8 + q_me) * 8 + lane % 8)
    planar = jnp.sqrt(qx * qx + qy * qy)
    magnitude = jnp.sqrt(planar * planar + qz * qz)
    coef[0] = magnitude * (qx * qz / (magnitude * planar))
    coef[1] = magnitude * (qy * qz / (magnitude * planar))
    coef[2] = magnitude * (-planar / magnitude)
    coef[3] = magnitude * (qy / planar)
    coef[4] = magnitude * (-qx / planar)
    coef[5] = 1.0 / (magnitude * magnitude + 1.0)
    pl.semaphore_wait(barrier, 29)
    table_copy(0).wait()

    def send(kind, t, source, target, peers, number, me):
        for k in range(1, number):
            device, slot = peers(k)
            pltpu.make_async_remote_copy(
                src_ref=source.at[slot], dst_ref=target.at[me],
                send_sem=send_x.at[kind, t], recv_sem=recv_x.at[kind, t],
                device_id=device, device_id_type=MESH_ID,
            ).start()
        target[me] = source[me]

    def descriptor(kind, t, source, target, number):
        return pltpu.make_async_remote_copy(
            src_ref=source.at[pl.ds(0, number - 1)], dst_ref=target.at[pl.ds(0, number - 1)],
            send_sem=send_x.at[kind, t], recv_sem=recv_x.at[kind, t],
            device_id=deep_peer(1)[0], device_id_type=MESH_ID,
        )

    def start_sum(slot):
        for k in range(1, 16):
            pltpu.make_async_remote_copy(
                src_ref=s_small.at[slot, 0], dst_ref=r_one.at[slot, p_me],
                send_sem=send_small.at[slot, 0], recv_sem=recv_small.at[slot, 0],
                device_id=wide_peer(k)[0], device_id_type=MESH_ID,
            ).start()
        r_one[slot, p_me] = s_small[slot, 0]

    def small_wait(slot, step, target, number):
        return pltpu.make_async_remote_copy(
            src_ref=target.at[slot, pl.ds(0, number - 1)], dst_ref=target.at[slot, pl.ds(0, number - 1)],
            send_sem=send_small.at[slot, step], recv_sem=recv_small.at[slot, step],
            device_id=deep_peer(1)[0], device_id_type=MESH_ID,
        )

    def middle_sum(slot):
        small_wait(slot, 0, r_one, 16).wait_recv()
        s_small[slot, 1] = jnp.sum(r_one[slot], axis=0)
        for k in range(1, 8):
            pltpu.make_async_remote_copy(
                src_ref=s_small.at[slot, 1], dst_ref=r_two.at[slot, q_me],
                send_sem=send_small.at[slot, 1], recv_sem=recv_small.at[slot, 1],
                device_id=deep_peer(k)[0], device_id_type=MESH_ID,
            ).start()
        r_two[slot, q_me] = s_small[slot, 1]

    def finish_sum(slot):
        small_wait(slot, 1, r_two, 8).wait_recv()
        return jnp.sum(r_two[slot], axis=0)

    def send_materials():
        material_copy.wait()
        for q in range(8):
            s_cell[q] = material[q].astype(F32).T.reshape(16, 8, N)
        me = xl_me * 8 + q_me
        for k in range(1, 16):
            device, xl, q = slab_peer(k)
            pltpu.make_async_remote_copy(
                src_ref=s_cell.at[q, xl * 8 + zb_me], dst_ref=r_cell.at[me],
                send_sem=cell_sem.at[0], recv_sem=cell_sem.at[1],
                device_id=device, device_id_type=MESH_ID,
            ).start()
        r_cell[me] = s_cell[q_me, p_me]

    cell_wait = pltpu.make_async_remote_copy(
        src_ref=r_cell.at[pl.ds(0, 15)], dst_ref=r_cell.at[pl.ds(0, 15)],
        send_sem=cell_sem.at[0], recv_sem=cell_sem.at[1],
        device_id=deep_peer(1)[0], device_id_type=MESH_ID,
    )

    def weigh_cells():
        cell_wait.wait_recv()
        kinds = jnp.dot(r_cell[...].reshape(N, N).astype(BF16), tab["order"][...], preferred_element_type=F32)
        met = (row // 8) == (lane // 8)
        placed = jnp.where(met, kinds, 0.0)
        for d in range(1, 16):
            moved = jnp.where(met, pltpu.roll(kinds, 8 * d, 1), 0.0)
            placed = placed + jnp.concatenate([moved[8 * d :], moved[: 8 * d]], 0)
        weights = jnp.zeros((N, N), F32)
        for kind in range(weight_ref.shape[0]):
            weights = weights + jnp.where(placed == float(kind), weight_ref[kind], 0.0)
        cell[...] = weights / CELLS

    def curl_and_send(kind, t, block):
        columns = []
        for c in range(3):
            halves = []
            for part in range(2):
                term = coef[c] * block[part]
                if c < 2:
                    term = term - coef[3 + c] * block[2 + part]
                halves.append(term)
            columns.append(jnp.concatenate(halves, 0))
        spread_x = rows_dot(tab["ta"], jnp.concatenate(columns, 1))
        op = kind // 4
        for c in range(3):
            s_a[op, t, :, c] = spread_x[:, c * N : (c + 1) * N].reshape(16, 2, 8, N)
        send(kind, t, s_a.at[op, t], r_a.at[op, t], wide_peer, 16, p_me)

    def z_stage(kind, t):
        op = kind // 4
        descriptor(kind - 1, t, s_a.at[op, t], r_a.at[op, t], 16).wait_recv()
        blocks = [r_a[op, t, pl.ds(xlo * 8, 8), c].reshape(N, N) for c in range(3) for xlo in range(2)]
        both = z_forward(tab, jnp.concatenate(blocks, 1))
        for k in range(6):
            for part in range(2):
                s_b[op, t, :, k, part] = both[k * 64 : (k + 1) * 64, part * N : (part + 1) * N].reshape(8, 8, N)
        send(kind, t, s_b.at[op, t], r_b.at[op, t], deep_peer, 8, q_me)

    def y_stage(kind, t):
        op = kind // 4
        descriptor(kind, t, s_b.at[op, t], r_b.at[op, t], 8).wait_recv()
        blocks = [r_b[op, t, :, pl.ds(2 * c, 2)].reshape(256, N) for c in range(3)]
        both = y_forward(tab, jnp.concatenate(blocks, 1))
        for c in range(3):
            for part in range(2):
                fields[t, c, part] = both[c * N : (c + 1) * N, part * N : (part + 1) * N].reshape(16, 8, N)

    def y_back_stage(t):
        weights = cell[...]
        rows = [
            jnp.concatenate([fields[t, c, part].reshape(N, N) * weights for part in range(2)], 1)
            for c in range(3)
        ]
        back = y_back(tab, jnp.concatenate(rows, 0))
        for c in range(3):
            s_c[t, :, pl.ds(2 * c, 2)] = back[:, c * N : (c + 1) * N].reshape(8, 2, 2, 8, N)
        send(2, t, s_c.at[t], r_c.at[t], deep_peer, 8, q_me)

    def z_back_stage(t):
        descriptor(2, t, s_c.at[t], r_c.at[t], 8).wait_recv()
        rows = [
            jnp.concatenate([r_c[t, :, k, part].reshape(64, N) for part in range(2)], 1) for k in range(6)
        ]
        back = z_back(tab, jnp.concatenate(rows, 0))
        for c in range(3):
            for xlo in range(2):
                k = 2 * c + xlo
                s_d[t, pl.ds(xlo * 8, 8), c] = back[:, k * N : (k + 1) * N].reshape(8, 2, 8, N)
        send(3, t, s_d.at[t], r_d.at[t], wide_peer, 16, p_me)

    def x_back_stage(t):
        descriptor(3, t, s_d.at[t], r_d.at[t], 16).wait_recv()
        columns = [r_d[t, :, c].reshape(256, N) for c in range(3)]
        back = rows_dot(tab["tat"], jnp.concatenate(columns, 1))
        for part in range(2):
            g = [back[part * N : (part + 1) * N, c * N : (c + 1) * N] for c in range(3)]
            image[t, 0, part] = (g[0] * coef[0] + g[1] * coef[1] + g[2] * coef[2]).reshape(16, 8, N)
            image[t, 1, part] = (-(g[0] * coef[3] + g[1] * coef[4])).reshape(16, 8, N)

    def gram(left, right, groups, slot, scale=None):
        def body(g, total):
            comp, m0 = g // 2, (g % 2) * 8
            left_cols = jnp.concatenate([left[:, comp, :, m0 + m].reshape(N, N) for m in range(8)], 1)
            if scale is None:
                right_cols = left_cols if right is left else jnp.concatenate(
                    [right[:, comp, :, m0 + m].reshape(N, N) for m in range(8)], 1
                )
            else:
                right_cols = []
                for m in range(8):
                    weight = scale[pl.ds(pl.multiple_of((m0 + m) * 8, 8), 8), :]
                    right_cols.append((right[:, comp, :, m0 + m] * weight[None, None]).reshape(N, N))
                right_cols = jnp.concatenate(right_cols, 1)
            lefts = jnp.concatenate(parts(left_cols), 0)
            rights = lefts if right_cols is left_cols else jnp.concatenate(parts(right_cols), 0)
            both = lax.dot_general(lefts, rights, (((1,), (1,)), ((), ())), preferred_element_type=F32)
            return total + (both[:N, :N] + ((both[:N, N:] + both[N:, :N]) + both[N:, N:]))

        total = lax.fori_loop(0, groups, body, jnp.zeros((N, N), F32))
        folded = exact_dot(tab["collect"][...], jnp.where(row % 8 == lane % 8, total, 0.0))
        sums = exact_dot(folded[:16], tab["place"][0]) + exact_dot(folded[16:], tab["place"][1])
        return pltpu.roll(sums, 16 * slot, 1) if slot else sums

    def mix():
        system = finish_sum(0)
        first_sum[...] = system
        rows16 = lax.broadcasted_iota(jnp.int32, (16, N), 0)
        for k in range(16):
            pivot = system[k : k + 1] / system[k : k + 1, k : k + 1]
            system = jnp.where(rows16 == k, pivot, system - system[:, k : k + 1] * pivot)
        wide = exact_dot(system, tab["spread"][...])
        spread_out = jnp.where(row % 8 == lane % 8, exact_dot(tab["gather"][...], wide).T, 0.0)
        mix_high, mix_low = parts(spread_out)
        mixing[:, :N] = mix_high
        mixing[:, N:] = mix_low

        def body(g, carry):
            comp, m0 = g // 2, (g % 2) * 8
            columns = jnp.concatenate([xt[:, comp, :, m0 + m].reshape(N, N) for m in range(8)], 1)
            mixed = rows_dot(mixing, columns)
            for m in range(8):
                search[:, comp, :, m0 + m] = mixed[:, m * N : (m + 1) * N].reshape(8, 2, 8, N)
            return carry

        lax.fori_loop(0, 4, body, 0)

    def out_copy(t):
        return pltpu.make_async_copy(out_stage.at[t], out_hbm.at[t], out_sem.at[t])

    def residual(t):
        block = []
        for comp in range(2):
            for part in range(2):
                left = (image[t, comp, part] - search[t, comp, part]).reshape(N, N) * coef[5]
                search[t, comp, part] = left.reshape(16, 8, N)
                block.append(left)
        curl_and_send(4, t, block)
        for comp in range(2):
            for part in range(2):
                out_stage[t, comp, part] = block[comp * 2 + part].T.reshape(16, 8, N)
        out_copy(t).start()

    def at(t, first, last, stage):
        @pl.when((t >= first) & (t < last))
        def _():
            stage()

    back, after = LAG_BACK, LAG_NEXT

    def step(t, carry):
        def load():
            band_copy(t).wait()
            for comp in range(2):
                for part in range(2):
                    xt[t, comp, part] = band_in[t, comp, part].reshape(N, N).T.reshape(16, 8, N)
            curl_and_send(0, t, [xt[t, c, r].reshape(N, N) for c in range(2) for r in range(2)])

        def rest_of_tables():
            for k in range(1, count):
                table_copy(k).wait()
            send_materials()

        def overlaps():
            s_small[0, 0] = gram(xt, xt, 4, 0)

        def overlaps_of_image():
            s_small[0, 0] = s_small[0, 0] + gram(fields, fields, 6, 1, cell)
            start_sum(0)

        def overlaps_of_search():
            s_small[1, 0] = gram(xt, search, 4, 0) + gram(search, search, 4, 1) + gram(search, image, 4, 2)

        at(t, 0, 8, load)
        at(t, 1, 2, rest_of_tables)
        at(t, 1, 9, lambda: z_stage(1, t - 1))
        at(t, back - 1, back, weigh_cells)
        at(t, back, back + 8, lambda: y_back_stage(t - back))
        at(t, back + 1, back + 9, lambda: z_back_stage(t - back - 1))
        at(t, 10, 11, lambda: middle_sum(0))
        at(t, back + 2, back + 10, lambda: x_back_stage(t - back - 2))
        at(t, after, after + 1, mix)
        at(t, after, after + 8, lambda: residual(t - after))
        at(t, after + 1, after + 9, lambda: z_stage(5, t - after - 1))
        at(t, 2, 10, lambda: y_stage(1, t - 2))
        at(t, 8, 9, overlaps)
        at(t, 9, 10, overlaps_of_image)
        at(t, after + 2, after + 10, lambda: y_stage(5, t - after - 2))
        at(t, after + 8, after + 9, overlaps_of_search)
        return carry

    lax.fori_loop(0, after + 10, step, 0)

    s_small[1, 0] = s_small[1, 0] + gram(fields, fields, 6, 3, cell)
    start_sum(1)
    middle_sum(1)
    second = finish_sum(1) / CELLS
    first = first_sum[...] / CELLS
    flipped = jnp.concatenate([second, jnp.zeros((N - 16, N), F32)], 0).T

    def joined(corner, right, below, last):
        return jnp.concatenate(
            [jnp.concatenate([corner, right], 1), jnp.concatenate([below, last], 1)], 0
        )

    corr_ref[0] = joined(first[:8, 0:8], second[:8, 0:8], flipped[0:8, :8], second[:8, 16:24])
    corr_ref[1] = joined(first[:8, 8:16], second[:8, 8:16], -flipped[8:16, :8], second[:8, 24:32])
    proj_ref[0] = joined(first[:8, 16:24], flipped[32:40, :8], second[:8, 32:40], second[:8, 48:56])
    proj_ref[1] = joined(first[:8, 24:32], -flipped[40:48, :8], second[:8, 40:48], second[:8, 56:64])

    def drain(t, carry):
        descriptor(0, t, s_a.at[0, t], r_a.at[0, t], 16).wait_send()
        descriptor(1, t, s_b.at[0, t], r_b.at[0, t], 8).wait_send()
        descriptor(2, t, s_c.at[t], r_c.at[t], 8).wait_send()
        descriptor(3, t, s_d.at[t], r_d.at[t], 16).wait_send()
        descriptor(4, t, s_a.at[1, t], r_a.at[1, t], 16).wait_send()
        descriptor(5, t, s_b.at[1, t], r_b.at[1, t], 8).wait_send()
        out_copy(t).wait()
        return carry

    lax.fori_loop(0, 8, drain, 0)
    cell_wait.wait_send()
    for slot in range(2):
        small_wait(slot, 0, r_one, 16).wait_send()
        small_wait(slot, 1, r_two, 8).wait_send()


def shards(band_block, material_grid, inverse_permittivity, bloch_index):
    table = {name: jnp.asarray(value) for name, value in tables().items()}
    vmem = pl.BlockSpec(memory_space=pltpu.VMEM)
    smem = pl.BlockSpec(memory_space=pltpu.SMEM)
    anywhere = pl.BlockSpec(memory_space=pl.ANY)
    block = (8, 2, 2, 16, 8, N)
    return pl.pallas_call(
        kernel,
        out_shape=(
            jax.ShapeDtypeStruct(band_block.shape, F32),
            jax.ShapeDtypeStruct((2, 16, 16), F32),
            jax.ShapeDtypeStruct((2, 16, 16), F32),
        ),
        in_specs=[smem, smem] + [anywhere] * (2 + len(NAMES)),
        out_specs=(anywhere, vmem, vmem),
        scratch_shapes=[
            pltpu.VMEM((6, N, N), F32),
            pltpu.VMEM(block, F32),
            pltpu.VMEM((8, N, N), jnp.int32),
            pltpu.VMEM((N, N), F32),
            pltpu.VMEM(block, F32),
            pltpu.VMEM(block, F32),
            pltpu.VMEM(block, F32),
            pltpu.VMEM(block, F32),
            pltpu.VMEM((8, 3, 2, 16, 8, N), F32),
            pltpu.VMEM((2, 8, 16, 3, 2, 8, N), F32),
            pltpu.VMEM((2, 8, 16, 3, 2, 8, N), F32),
            pltpu.VMEM((2, 8, 8, 6, 2, 8, N), F32),
            pltpu.VMEM((2, 8, 8, 6, 2, 8, N), F32),
            pltpu.VMEM((8, 8, 6, 2, 8, N), F32),
            pltpu.VMEM((8, 8, 6, 2, 8, N), F32),
            pltpu.VMEM((8, 16, 3, 2, 8, N), F32),
            pltpu.VMEM((8, 16, 3, 2, 8, N), F32),
            pltpu.VMEM((8, 16, 8, N), F32),
            pltpu.VMEM((16, 8, N), F32),
            pltpu.VMEM((2, 2, 16, N), F32),
            pltpu.VMEM((2, 16, 16, N), F32),
            pltpu.VMEM((2, 8, 16, N), F32),
            pltpu.VMEM((16, N), F32),
            pltpu.VMEM((N, 2 * N), BF16),
            pltpu.SemaphoreType.DMA((6, 8)),
            pltpu.SemaphoreType.DMA((6, 8)),
            pltpu.SemaphoreType.DMA((2, 2)),
            pltpu.SemaphoreType.DMA((2, 2)),
            pltpu.SemaphoreType.DMA((3,)),
            pltpu.SemaphoreType.DMA((8,)),
            pltpu.SemaphoreType.DMA((len(NAMES),)),
            pltpu.SemaphoreType.DMA((8,)),
        ] + [pltpu.VMEM(table[name].shape, table[name].dtype) for name in NAMES],
        compiler_params=pltpu.CompilerParams(
            collective_id=0, has_side_effects=True, vmem_limit_bytes=63 * 1024 * 1024
        ),
    )(bloch_index, inverse_permittivity, band_block, material_grid, *[table[name] for name in NAMES])


def solution(mesh):
    finer = Mesh(
        mesh.devices.reshape(4, 2, 2, 4, 2), ("band_0", "band_1", "slab_0", "slab_1", "slab_2")
    )
    placed = (P(None, None, None, BAND, SLAB, None), P(SLAB, None, None), P(), P())
    return jax.shard_map(
        shards,
        mesh=finer,
        in_specs=placed,
        out_specs=(P(None, None, None, BAND, SLAB, None), P(), P()),
        check_vma=False,
    )
```

```python
import functools
import math

import jax
import jax.numpy as jnp
import numpy as np
from jax import lax
from jax.experimental import pallas as pl
from jax.experimental.pallas import tpu as pltpu
from jax.sharding import Mesh
from jax.sharding import PartitionSpec as P

KPOINTS = 8
N = 128
CELLS = N * N * N
BANDS = 8
BAND = ("band_0", "band_1")
SLAB = ("slab_0", "slab_1", "slab_2")
HIGHEST = lax.Precision.HIGHEST
F32 = jnp.float32
BF16 = jnp.bfloat16


def _rot(angle):
    c, s = np.cos(angle), np.sin(angle)
    return np.stack([np.stack([c, -s]), np.stack([s, c])])


def _halves(table):
    high = table.astype(BF16)
    low = (table - high.astype(np.float64)).astype(BF16)
    return high, low


def _left(table):
    high, low = _halves(table)
    return np.concatenate([high, low], 1)


def _right(table):
    high, low = _halves(table)
    return np.concatenate([high, low], 0)


def tables():
    tau = 2.0 * math.pi
    i128, i16, i8 = np.arange(128), np.arange(16), np.arange(8)
    r = _rot(tau / 128 * (i128[:, None] * i128[None, :] % 128))
    ta = r.reshape(2, 2, 16, 8, 128).transpose(2, 0, 3, 1, 4).reshape(256, 256)
    r = _rot(tau / 8 * (i8[:, None] * i8[None, :] % 8))
    kz = np.einsum("abzs,xy->azxsby", r, np.eye(8)).reshape(128, 128)
    r = _rot(tau / 16 * (i16[:, None] * i16[None, :] % 16))
    wz = np.einsum("abos,xy->bsxaoy", r, np.eye(8)).reshape(256, 256)
    r = _rot(tau / 16 * (i16[:, None] * i16[None, :] % 16)).reshape(2, 2, 16, 2, 8)
    ky = np.einsum("abolq,xy->aoxqlby", r, np.eye(8)).reshape(256, 256)
    r = _rot(tau / 8 * (i8[:, None] * i8[None, :] % 8))
    wy = np.einsum("abos,xy->bxsayo", r, np.eye(16)).reshape(256, 256)
    lane = np.arange(128)
    az = tau / 128 * ((np.arange(64) // 8)[:, None] * (lane // 8)[None, :])
    ay = tau / 128 * ((np.arange(128) // 8)[:, None] * (lane % 8)[None, :])
    twz = np.stack([np.cos(az), np.sin(az)]).astype(np.float32)
    twy = np.stack([np.cos(ay), np.sin(ay)]).astype(np.float32)
    gather = np.zeros((128, 16), np.float32)
    for band in range(8):
        for part in range(2):
            gather[(band * 2 + part) * 8 : (band * 2 + part + 1) * 8, part * 8 + band] = 1.0
    turn = np.zeros((16, 16), np.float32)
    turn[:8, 8:] = np.eye(8)
    turn[8:, :8] = -np.eye(8)
    turned = gather @ turn.T
    collect = np.concatenate([gather.T[:8], turned.T[:8]], 0)
    place = np.zeros((2, 128, 128), np.float32)
    place[0, :, :16] = gather
    place[1, :, :16] = turned
    spread = np.zeros((128, 128), np.float32)
    spread[16:32] = gather.T
    order = np.zeros((128, 128), np.float32)
    order[lane, lane % 16 * 8 + lane // 16] = 1.0
    return dict(
        ta=_left(ta), tat=_left(ta.T), kz=_left(kz), kzt=_left(kz.T), ky=_left(ky), kyt=_left(ky.T),
        wz=_right(wz), wzt=_right(wz.T), wy=_right(wy), wyt=_right(wy.T),
        twz=twz, twy=twy, collect=collect, place=place, spread=spread, gather=gather, order=order.astype(BF16),
    )


NAMES = ("ta", "tat", "kz", "kzt", "ky", "kyt", "wz", "wzt", "wy", "wyt", "twz", "twy",
         "collect", "place", "spread", "gather", "order")


def parts(x):
    high = x.astype(BF16)
    low = (x - high.astype(F32)).astype(BF16)
    return high, low


def rows_dot(table, x):
    high, low = parts(x)
    k = x.shape[0]
    return jnp.dot(
        jnp.concatenate([table[:, :k], table[:, :k], table[:, k:]], 1),
        jnp.concatenate([high, low, high], 0),
        preferred_element_type=F32,
    )


def lanes_dot(x, table):
    high, low = parts(x)
    k = x.shape[1]
    return jnp.dot(
        jnp.concatenate([high, low, high], 1),
        jnp.concatenate([table[:k], table[:k], table[k:]], 0),
        preferred_element_type=F32,
    )


def exact_dot(x, y):
    return jnp.dot(x, y, precision=HIGHEST, preferred_element_type=F32)


def turn_by(re, im, cosine, sine):
    return re * cosine - im * sine, re * sine + im * cosine


def turn_back(re, im, cosine, sine):
    return re * cosine + im * sine, im * cosine - re * sine


def cut(x, size, axis=1):
    return [lax.slice_in_dim(x, k, k + size, axis=axis) for k in range(0, x.shape[axis], size)]


def z_forward(tab, blocks):
    mixed = rows_dot(tab["kz"], blocks)
    cosine, sine = tab["twz"][0], tab["twz"][1]
    pairs = [turn_by(b[:64], b[64:], cosine, sine) for b in cut(mixed, 128)]
    both = jnp.concatenate(
        [jnp.concatenate([a for a, _ in pairs], 0), jnp.concatenate([b for _, b in pairs], 0)], 1
    )
    return lanes_dot(both, tab["wz"])


def z_back(tab, both):
    mixed = lanes_dot(both, tab["wzt"])
    cosine, sine = tab["twz"][0], tab["twz"][1]
    blocks = []
    for b in cut(mixed, 64, 0):
        re, im = turn_back(b[:, :128], b[:, 128:], cosine, sine)
        blocks.append(jnp.concatenate([re, im], 0))
    return rows_dot(tab["kzt"], jnp.concatenate(blocks, 1))


def y_forward(tab, blocks):
    mixed = rows_dot(tab["ky"], blocks)
    cosine, sine = tab["twy"][0], tab["twy"][1]
    pairs = [turn_by(b[:128], b[128:], cosine, sine) for b in cut(mixed, 128)]
    both = jnp.concatenate(
        [jnp.concatenate([a for a, _ in pairs], 0), jnp.concatenate([b for _, b in pairs], 0)], 1
    )
    return lanes_dot(both, tab["wy"])


def y_back(tab, both):
    mixed = lanes_dot(both, tab["wyt"])
    cosine, sine = tab["twy"][0], tab["twy"][1]
    blocks = []
    for b in cut(mixed, 128, 0):
        re, im = turn_back(b[:, :128], b[:, 128:], cosine, sine)
        blocks.append(jnp.concatenate([re, im], 0))
    return rows_dot(tab["kyt"], jnp.concatenate(blocks, 1))


def axis_values(length, weight, fraction, indices):
    signed = jnp.where(indices >= length // 2, indices - length, indices).astype(F32)
    return 2.0 * math.pi / length * (signed + weight * fraction)


START = dict(A=(0, 2), B=(2, 1), C=(4, 1), Cb=(6, 1), Bb=(9, 1), Ab=(15, 2), R=(15, 2), B2=(17, 1), C2=(22, 1))
ONCE = dict(cells=0, tables=1, gS=5, weigh=5, gH=12, m=13, mix=15, gJ1=21, gJ2=25, gJ3=23, gP=29)
ORDER = ("B", "C2", "gJ1", "gP", "gJ2", "A", "cells", "tables", "B2", "gH", "Ab", "Bb", "gJ3", "m",
         "weigh", "Cb", "mix", "gS", "R", "C")
MESH_ID = pl.DeviceIdType.MESH


def kernel(bloch_ref, weight_ref, band_hbm, material_hbm, *refs):
    count = len(NAMES)
    table_hbm = refs[:count]
    (out_hbm, corr_ref, proj_ref, coef, band_in, material, cell, xt, image, search, out_stage, fields,
     s_a, r_a, s_b, r_b, s_c, r_c, s_d, r_d, s_cell, r_cell, s_small, r_one, r_two, first_sum, mixing,
     send_x, recv_x, send_small, recv_small, cell_sem, in_sem, table_sem, out_sem) = refs[count : -count]
    tab = dict(zip(NAMES, refs[-count:]))
    y_me, xh_me, xl_me = (lax.axis_index(a) for a in ("band_0", "band_1", "slab_0"))
    z_me, c_me = lax.axis_index("slab_1"), lax.axis_index("slab_2")
    zb_me = y_me * 2 + xh_me
    p_me = xl_me * 8 + zb_me
    q_me = z_me * 2 + c_me
    x_me = xh_me * 2 + xl_me

    def wide_peer(k):
        y = (y_me + k // 4) % 4
        x = (x_me + k % 4) % 4
        return {"band_0": y, "band_1": x // 2, "slab_0": x % 2}, (x % 2) * 8 + y * 2 + x // 2

    def deep_peer(k):
        z = (z_me + k // 2) % 4
        c = (c_me + k % 2) % 2
        return {"slab_1": z, "slab_2": c}, z * 2 + c

    def slab_peer(k):
        xl = (xl_me + k // 8) % 2
        z = (z_me + k // 2 % 4) % 4
        c = (c_me + k % 2) % 2
        return {"slab_0": xl, "slab_1": z, "slab_2": c}, xl, z * 2 + c

    def band_copy(t):
        return pltpu.make_async_copy(band_hbm.at[t], band_in.at[t], in_sem.at[t])

    def table_copy(k):
        return pltpu.make_async_copy(table_hbm[k], tab[NAMES[k]], table_sem.at[k])

    material_copy = pltpu.make_async_copy(material_hbm, material, cell_sem.at[2])
    band_copy(0).start()
    table_copy(0).start()
    for t in range(1, 8):
        band_copy(t).start()
    for k in range(1, count):
        table_copy(k).start()
    material_copy.start()

    barrier = pltpu.get_barrier_semaphore()
    for k in range(1, 16):
        pl.semaphore_signal(barrier, inc=1, device_id=wide_peer(k)[0], device_id_type=MESH_ID)
    for k in range(1, 8):
        pl.semaphore_signal(barrier, inc=1, device_id=deep_peer(k)[0], device_id_type=MESH_ID)
    for k in range(9, 16):
        pl.semaphore_signal(barrier, inc=1, device_id=slab_peer(k)[0], device_id_type=MESH_ID)

    fraction = (bloch_ref[0].astype(F32) + 1.0) / KPOINTS
    row = lax.broadcasted_iota(jnp.int32, (N, N), 0)
    lane = lax.broadcasted_iota(jnp.int32, (N, N), 1)
    qx = axis_values(N, 0.5, fraction, row)
    qz = axis_values(N, 0.2, fraction, zb_me * 16 + lane // 8)
    qy = axis_values(N, 0.35, fraction, (xl_me * 8 + q_me) * 8 + lane % 8)
    planar = jnp.sqrt(qx * qx + qy * qy)
    magnitude = jnp.sqrt(planar * planar + qz * qz)
    coef[0] = magnitude * (qx * qz / (magnitude * planar))
    coef[1] = magnitude * (qy * qz / (magnitude * planar))
    coef[2] = magnitude * (-planar / magnitude)
    coef[3] = magnitude * (qy / planar)
    coef[4] = magnitude * (-qx / planar)
    coef[5] = 1.0 / (magnitude * magnitude + 1.0)
    pl.semaphore_wait(barrier, 29)
    table_copy(0).wait()

    def send(kind, t, source, target, peers, number, me):
        for k in range(1, number):
            device, slot = peers(k)
            pltpu.make_async_remote_copy(
                src_ref=source.at[slot], dst_ref=target.at[me],
                send_sem=send_x.at[kind, t], recv_sem=recv_x.at[kind, t],
                device_id=device, device_id_type=MESH_ID,
            ).start()
        target[me] = source[me]

    def descriptor(kind, t, source, target, number):
        return pltpu.make_async_remote_copy(
            src_ref=source.at[pl.ds(0, number - 1)], dst_ref=target.at[pl.ds(0, number - 1)],
            send_sem=send_x.at[kind, t], recv_sem=recv_x.at[kind, t],
            device_id=deep_peer(1)[0], device_id_type=MESH_ID,
        )

    def start_sum(slot):
        for k in range(1, 16):
            pltpu.make_async_remote_copy(
                src_ref=s_small.at[slot, 0], dst_ref=r_one.at[slot, p_me],
                send_sem=send_small.at[slot, 0], recv_sem=recv_small.at[slot, 0],
                device_id=wide_peer(k)[0], device_id_type=MESH_ID,
            ).start()
        r_one[slot, p_me] = s_small[slot, 0]

    def small_wait(slot, step, target, number):
        return pltpu.make_async_remote_copy(
            src_ref=target.at[slot, pl.ds(0, number - 1)], dst_ref=target.at[slot, pl.ds(0, number - 1)],
            send_sem=send_small.at[slot, step], recv_sem=recv_small.at[slot, step],
            device_id=deep_peer(1)[0], device_id_type=MESH_ID,
        )

    def middle_sum(slot):
        small_wait(slot, 0, r_one, 16).wait_recv()
        s_small[slot, 1] = jnp.sum(r_one[slot], axis=0)
        for k in range(1, 8):
            pltpu.make_async_remote_copy(
                src_ref=s_small.at[slot, 1], dst_ref=r_two.at[slot, q_me],
                send_sem=send_small.at[slot, 1], recv_sem=recv_small.at[slot, 1],
                device_id=deep_peer(k)[0], device_id_type=MESH_ID,
            ).start()
        r_two[slot, q_me] = s_small[slot, 1]

    def finish_sum(slot):
        small_wait(slot, 1, r_two, 8).wait_recv()
        return jnp.sum(r_two[slot], axis=0)

    def send_materials():
        material_copy.wait()
        for q in range(8):
            s_cell[q] = material[q].astype(F32).T.reshape(16, 8, N)
        me = xl_me * 8 + q_me
        for k in range(1, 16):
            device, xl, q = slab_peer(k)
            pltpu.make_async_remote_copy(
                src_ref=s_cell.at[q, xl * 8 + zb_me], dst_ref=r_cell.at[me],
                send_sem=cell_sem.at[0], recv_sem=cell_sem.at[1],
                device_id=device, device_id_type=MESH_ID,
            ).start()
        r_cell[me] = s_cell[q_me, p_me]

    cell_wait = pltpu.make_async_remote_copy(
        src_ref=r_cell.at[pl.ds(0, 15)], dst_ref=r_cell.at[pl.ds(0, 15)],
        send_sem=cell_sem.at[0], recv_sem=cell_sem.at[1],
        device_id=deep_peer(1)[0], device_id_type=MESH_ID,
    )

    def weigh_cells():
        cell_wait.wait_recv()
        kinds = jnp.dot(r_cell[...].reshape(N, N).astype(BF16), tab["order"][...], preferred_element_type=F32)
        met = (row // 8) == (lane // 8)
        placed = jnp.where(met, kinds, 0.0)
        for d in range(1, 16):
            moved = jnp.where(met, pltpu.roll(kinds, 8 * d, 1), 0.0)
            placed = placed + jnp.concatenate([moved[8 * d :], moved[: 8 * d]], 0)
        weights = jnp.zeros((N, N), F32)
        for kind in range(weight_ref.shape[0]):
            weights = weights + jnp.where(placed == float(kind), weight_ref[kind], 0.0)
        cell[...] = weights / CELLS

    def curl_and_send(kind, t, block):
        columns = []
        for c in range(3):
            halves = []
            for part in range(2):
                term = coef[c] * block[part]
                if c < 2:
                    term = term - coef[3 + c] * block[2 + part]
                halves.append(term)
            columns.append(jnp.concatenate(halves, 0))
        spread_x = rows_dot(tab["ta"], jnp.concatenate(columns, 1))
        op = kind // 4
        for c in range(3):
            s_a[op, t, :, c] = spread_x[:, c * N : (c + 1) * N].reshape(16, 2, 8, N)
        send(kind, t, s_a.at[op, t], r_a.at[op, t], wide_peer, 16, p_me)

    def z_stage(kind, t):
        op = kind // 4
        descriptor(kind - 1, t, s_a.at[op, t], r_a.at[op, t], 16).wait_recv()
        blocks = [r_a[op, t, pl.ds(xlo * 8, 8), c].reshape(N, N) for c in range(3) for xlo in range(2)]
        both = z_forward(tab, jnp.concatenate(blocks, 1))
        for k in range(6):
            for part in range(2):
                s_b[op, t, :, k, part] = both[k * 64 : (k + 1) * 64, part * N : (part + 1) * N].reshape(8, 8, N)
        send(kind, t, s_b.at[op, t], r_b.at[op, t], deep_peer, 8, q_me)

    def y_stage(kind, t):
        op = kind // 4
        descriptor(kind, t, s_b.at[op, t], r_b.at[op, t], 8).wait_recv()
        blocks = [r_b[op, t, :, pl.ds(2 * c, 2)].reshape(256, N) for c in range(3)]
        both = y_forward(tab, jnp.concatenate(blocks, 1))
        for c in range(3):
            for part in range(2):
                fields[t, c, part] = both[c * N : (c + 1) * N, part * N : (part + 1) * N].reshape(16, 8, N)

    def y_back_stage(t):
        weights = cell[...]
        rows = [
            jnp.concatenate([fields[t, c, part].reshape(N, N) * weights for part in range(2)], 1)
            for c in range(3)
        ]
        back = y_back(tab, jnp.concatenate(rows, 0))
        for c in range(3):
            s_c[t, :, pl.ds(2 * c, 2)] = back[:, c * N : (c + 1) * N].reshape(8, 2, 2, 8, N)
        send(2, t, s_c.at[t], r_c.at[t], deep_peer, 8, q_me)

    def z_back_stage(t):
        descriptor(2, t, s_c.at[t], r_c.at[t], 8).wait_recv()
        rows = [
            jnp.concatenate([r_c[t, :, k, part].reshape(64, N) for part in range(2)], 1) for k in range(6)
        ]
        back = z_back(tab, jnp.concatenate(rows, 0))
        for c in range(3):
            for xlo in range(2):
                k = 2 * c + xlo
                s_d[t, pl.ds(xlo * 8, 8), c] = back[:, k * N : (k + 1) * N].reshape(8, 2, 8, N)
        send(3, t, s_d.at[t], r_d.at[t], wide_peer, 16, p_me)

    def x_back_stage(t):
        descriptor(3, t, s_d.at[t], r_d.at[t], 16).wait_recv()
        columns = [r_d[t, :, c].reshape(256, N) for c in range(3)]
        back = rows_dot(tab["tat"], jnp.concatenate(columns, 1))
        for part in range(2):
            g = [back[part * N : (part + 1) * N, c * N : (c + 1) * N] for c in range(3)]
            image[t, 0, part] = (g[0] * coef[0] + g[1] * coef[1] + g[2] * coef[2]).reshape(16, 8, N)
            image[t, 1, part] = (-(g[0] * coef[3] + g[1] * coef[4])).reshape(16, 8, N)

    def gram(left, right, groups, slot, scale=None):
        def body(g, total):
            comp, m0 = g // 2, (g % 2) * 8
            left_cols = jnp.concatenate([left[:, comp, :, m0 + m].reshape(N, N) for m in range(8)], 1)
            if scale is None:
                right_cols = left_cols if right is left else jnp.concatenate(
                    [right[:, comp, :, m0 + m].reshape(N, N) for m in range(8)], 1
                )
            else:
                right_cols = []
                for m in range(8):
                    weight = scale[pl.ds(pl.multiple_of((m0 + m) * 8, 8), 8), :]
                    right_cols.append((right[:, comp, :, m0 + m] * weight[None, None]).reshape(N, N))
                right_cols = jnp.concatenate(right_cols, 1)
            lefts = jnp.concatenate(parts(left_cols), 0)
            rights = lefts if right_cols is left_cols else jnp.concatenate(parts(right_cols), 0)
            both = lax.dot_general(lefts, rights, (((1,), (1,)), ((), ())), preferred_element_type=F32)
            return total + (both[:N, :N] + ((both[:N, N:] + both[N:, :N]) + both[N:, N:]))

        total = lax.fori_loop(0, groups, body, jnp.zeros((N, N), F32))
        folded = exact_dot(tab["collect"][...], jnp.where(row % 8 == lane % 8, total, 0.0))
        sums = exact_dot(folded[:8], tab["place"][0]) + exact_dot(folded[8:], tab["place"][1])
        return pltpu.roll(sums, 16 * slot, 1) if slot else sums

    def mix():
        top = finish_sum(0)
        first_sum[...] = top
        left = lax.broadcasted_iota(jnp.int32, (8, N), 1) % 16 < 8
        below = jnp.where(left, -pltpu.roll(top, N - 8, 1), pltpu.roll(top, 8, 1))
        system = jnp.concatenate([top, below], 0)
        rows16 = lax.broadcasted_iota(jnp.int32, (16, N), 0)
        for k in range(16):
            pivot = system[k : k + 1] / system[k : k + 1, k : k + 1]
            system = jnp.where(rows16 == k, pivot, system - system[:, k : k + 1] * pivot)
        wide = exact_dot(system, tab["spread"][...])
        spread_out = jnp.where(row % 8 == lane % 8, exact_dot(tab["gather"][...], wide).T, 0.0)
        mix_high, mix_low = parts(spread_out)
        mixing[:, :N] = mix_high
        mixing[:, N:] = mix_low

        def body(g, carry):
            comp, m0 = g // 2, (g % 2) * 8
            columns = jnp.concatenate([xt[:, comp, :, m0 + m].reshape(N, N) for m in range(8)], 1)
            mixed = rows_dot(mixing, columns)
            for m in range(8):
                search[:, comp, :, m0 + m] = mixed[:, m * N : (m + 1) * N].reshape(8, 2, 8, N)
            return carry

        lax.fori_loop(0, 4, body, 0)

    def out_copy(t):
        return pltpu.make_async_copy(out_stage.at[t], out_hbm.at[t], out_sem.at[t])

    def residual(t):
        block = []
        for comp in range(2):
            for part in range(2):
                left = (image[t, comp, part] - search[t, comp, part]).reshape(N, N) * coef[5]
                search[t, comp, part] = left.reshape(16, 8, N)
                block.append(left)
        curl_and_send(4, t, block)
        for comp in range(2):
            for part in range(2):
                out_stage[t, comp, part] = block[comp * 2 + part].T.reshape(16, 8, N)
        out_copy(t).start()

    def load(t):
        band_copy(t).wait()
        for comp in range(2):
            for part in range(2):
                xt[t, comp, part] = band_in[t, comp, part].reshape(N, N).T.reshape(16, 8, N)
        curl_and_send(0, t, [xt[t, c, r].reshape(N, N) for c in range(2) for r in range(2)])

    def rest_of_tables():
        for k in range(1, count):
            table_copy(k).wait()

    def overlaps():
        s_small[0, 0] = gram(xt, xt, 4, 0)

    def overlaps_of_image():
        s_small[0, 0] = s_small[0, 0] + gram(fields, fields, 6, 1, cell)
        start_sum(0)

    def first_overlaps_of_search():
        s_small[1, 0] = gram(xt, search, 4, 0)

    def add_overlaps(left, right, groups, slot, scale=None):
        s_small[1, 0] = s_small[1, 0] + gram(left, right, groups, slot, scale)

    stages = dict(
        A=load,
        B=lambda t: z_stage(1, t),
        C=lambda t: y_stage(1, t),
        Cb=y_back_stage,
        Bb=z_back_stage,
        Ab=x_back_stage,
        R=residual,
        B2=lambda t: z_stage(5, t),
        C2=lambda t: y_stage(5, t),
    )
    once = dict(
        cells=send_materials,
        tables=rest_of_tables,
        weigh=weigh_cells,
        gS=overlaps,
        gH=overlaps_of_image,
        m=lambda: middle_sum(0),
        mix=mix,
        gJ1=first_overlaps_of_search,
        gJ2=lambda: add_overlaps(search, search, 4, 1),
        gJ3=lambda: add_overlaps(search, image, 4, 2),
        gP=lambda: add_overlaps(fields, fields, 6, 3, cell),
    )

    def run(t, name):
        if name in ONCE:
            pl.when(t == ONCE[name])(once[name])
            return
        first, rate = START[name]

        @pl.when((t >= first) & (t < first + 8 // rate))
        def _():
            if rate == 1:
                stages[name](t - first)
            else:
                def body(k, carry):
                    stages[name]((t - first) * rate + k)
                    return carry

                lax.fori_loop(0, rate, body, 0)

    def step(t, carry):
        for name in ORDER:
            run(t, name)
        return carry

    lax.fori_loop(0, ONCE["gP"] + 1, step, 0)

    start_sum(1)
    middle_sum(1)
    second = finish_sum(1) / CELLS
    first = first_sum[...] / CELLS
    flipped = jnp.concatenate([second, jnp.zeros((N - 8, N), F32)], 0).T

    def joined(corner, right, below, last):
        return jnp.concatenate(
            [jnp.concatenate([corner, right], 1), jnp.concatenate([below, last], 1)], 0
        )

    corr_ref[0] = joined(first[:8, 0:8], second[:8, 0:8], flipped[0:8, :8], second[:8, 16:24])
    corr_ref[1] = joined(first[:8, 8:16], second[:8, 8:16], -flipped[8:16, :8], second[:8, 24:32])
    proj_ref[0] = joined(first[:8, 16:24], flipped[32:40, :8], second[:8, 32:40], second[:8, 48:56])
    proj_ref[1] = joined(first[:8, 24:32], -flipped[40:48, :8], second[:8, 40:48], second[:8, 56:64])

    def drain(t, carry):
        descriptor(0, t, s_a.at[0, t], r_a.at[0, t], 16).wait_send()
        descriptor(1, t, s_b.at[0, t], r_b.at[0, t], 8).wait_send()
        descriptor(2, t, s_c.at[t], r_c.at[t], 8).wait_send()
        descriptor(3, t, s_d.at[t], r_d.at[t], 16).wait_send()
        descriptor(4, t, s_a.at[1, t], r_a.at[1, t], 16).wait_send()
        descriptor(5, t, s_b.at[1, t], r_b.at[1, t], 8).wait_send()
        out_copy(t).wait()
        return carry

    lax.fori_loop(0, 8, drain, 0)
    cell_wait.wait_send()
    for slot in range(2):
        small_wait(slot, 0, r_one, 16).wait_send()
        small_wait(slot, 1, r_two, 8).wait_send()


def shards(band_block, material_grid, inverse_permittivity, bloch_index):
    table = {name: jnp.asarray(value) for name, value in tables().items()}
    vmem = pl.BlockSpec(memory_space=pltpu.VMEM)
    smem = pl.BlockSpec(memory_space=pltpu.SMEM)
    anywhere = pl.BlockSpec(memory_space=pl.ANY)
    block = (8, 2, 2, 16, 8, N)
    return pl.pallas_call(
        kernel,
        out_shape=(
            jax.ShapeDtypeStruct(band_block.shape, F32),
            jax.ShapeDtypeStruct((2, 16, 16), F32),
            jax.ShapeDtypeStruct((2, 16, 16), F32),
        ),
        in_specs=[smem, smem] + [anywhere] * (2 + len(NAMES)),
        out_specs=(anywhere, vmem, vmem),
        scratch_shapes=[
            pltpu.VMEM((6, N, N), F32),
            pltpu.VMEM(block, F32),
            pltpu.VMEM((8, N, N), jnp.int32),
            pltpu.VMEM((N, N), F32),
            pltpu.VMEM(block, F32),
            pltpu.VMEM(block, F32),
            pltpu.VMEM(block, F32),
            pltpu.VMEM(block, F32),
            pltpu.VMEM((8, 3, 2, 16, 8, N), F32),
            pltpu.VMEM((2, 8, 16, 3, 2, 8, N), F32),
            pltpu.VMEM((2, 8, 16, 3, 2, 8, N), F32),
            pltpu.VMEM((2, 8, 8, 6, 2, 8, N), F32),
            pltpu.VMEM((2, 8, 8, 6, 2, 8, N), F32),
            pltpu.VMEM((8, 8, 6, 2, 8, N), F32),
            pltpu.VMEM((8, 8, 6, 2, 8, N), F32),
            pltpu.VMEM((8, 16, 3, 2, 8, N), F32),
            pltpu.VMEM((8, 16, 3, 2, 8, N), F32),
            pltpu.VMEM((8, 16, 8, N), F32),
            pltpu.VMEM((16, 8, N), F32),
            pltpu.VMEM((2, 2, 8, N), F32),
            pltpu.VMEM((2, 16, 8, N), F32),
            pltpu.VMEM((2, 8, 8, N), F32),
            pltpu.VMEM((8, N), F32),
            pltpu.VMEM((N, 2 * N), BF16),
            pltpu.SemaphoreType.DMA((6, 8)),
            pltpu.SemaphoreType.DMA((6, 8)),
            pltpu.SemaphoreType.DMA((2, 2)),
            pltpu.SemaphoreType.DMA((2, 2)),
            pltpu.SemaphoreType.DMA((3,)),
            pltpu.SemaphoreType.DMA((8,)),
            pltpu.SemaphoreType.DMA((len(NAMES),)),
            pltpu.SemaphoreType.DMA((8,)),
        ] + [pltpu.VMEM(table[name].shape, table[name].dtype) for name in NAMES],
        compiler_params=pltpu.CompilerParams(
            collective_id=0, has_side_effects=True, vmem_limit_bytes=63 * 1024 * 1024
        ),
    )(bloch_index, inverse_permittivity, band_block, material_grid, *[table[name] for name in NAMES])


def solution(mesh):
    finer = Mesh(
        mesh.devices.reshape(4, 2, 2, 4, 2), ("band_0", "band_1", "slab_0", "slab_1", "slab_2")
    )
    placed = (P(None, None, None, BAND, SLAB, None), P(SLAB, None, None), P(), P())
    return jax.shard_map(
        shards,
        mesh=finer,
        in_specs=placed,
        out_specs=(P(None, None, None, BAND, SLAB, None), P(), P()),
        check_vma=False,
    )
```

```python
import functools
import math

import jax
import jax.numpy as jnp
import numpy as np
from jax import lax
from jax.experimental import pallas as pl
from jax.experimental.pallas import tpu as pltpu
from jax.sharding import Mesh
from jax.sharding import PartitionSpec as P

KPOINTS = 8
N = 128
CELLS = N * N * N
BANDS = 8
BAND = ("band_0", "band_1")
SLAB = ("slab_0", "slab_1", "slab_2")
HIGHEST = lax.Precision.HIGHEST
F32 = jnp.float32
BF16 = jnp.bfloat16


def _rot(angle):
    c, s = np.cos(angle), np.sin(angle)
    return np.stack([np.stack([c, -s]), np.stack([s, c])])


def _halves(table):
    high = table.astype(BF16)
    low = (table - high.astype(np.float64)).astype(BF16)
    return high, low


def _left(table):
    high, low = _halves(table)
    return np.concatenate([high, low], 1)


def _right(table):
    high, low = _halves(table)
    return np.concatenate([high, low], 0)


def tables():
    tau = 2.0 * math.pi
    i128, i16, i8 = np.arange(128), np.arange(16), np.arange(8)
    r = _rot(tau / 128 * (i128[:, None] * i128[None, :] % 128))
    ta = r.reshape(2, 2, 16, 8, 128).transpose(2, 0, 3, 1, 4).reshape(256, 256)
    r = _rot(tau / 16 * (i16[:, None] * i16[None, :] % 16))
    wz = np.einsum("abos,xy->bsxaoy", r, np.eye(8)).reshape(256, 256)
    r = _rot(tau / 8 * (i8[:, None] * i8[None, :] % 8))
    wy = np.einsum("abos,xy->bxsayo", r, np.eye(16)).reshape(256, 256)
    lane = np.arange(128)
    az = tau / 128 * ((np.arange(64) // 8)[:, None] * (lane // 8)[None, :])
    ay = tau / 128 * ((np.arange(128) // 8)[:, None] * (lane % 8)[None, :])
    twz = np.stack([np.cos(az), np.sin(az)]).astype(np.float32)
    twy = np.stack([np.cos(ay), np.sin(ay)]).astype(np.float32)
    gather = np.zeros((128, 16), np.float32)
    for band in range(8):
        for part in range(2):
            gather[(band * 2 + part) * 8 : (band * 2 + part + 1) * 8, part * 8 + band] = 1.0
    turn = np.zeros((16, 16), np.float32)
    turn[:8, 8:] = np.eye(8)
    turn[8:, :8] = -np.eye(8)
    turned = gather @ turn.T
    collect = np.concatenate([gather.T[:8], turned.T[:8]], 0)
    place = np.zeros((2, 128, 128), np.float32)
    place[0, :, :16] = gather
    place[1, :, :16] = turned
    spread = np.zeros((128, 128), np.float32)
    spread[16:32] = gather.T
    order = np.zeros((128, 128), np.float32)
    order[lane, lane % 16 * 8 + lane // 16] = 1.0
    return dict(
        ta=_left(ta), tat=_left(ta.T),
        wz=_right(wz), wzt=_right(wz.T), wy=_right(wy), wyt=_right(wy.T),
        twz=twz, twy=twy, collect=collect, place=place, spread=spread, gather=gather, order=order.astype(BF16),
    )


NAMES = ("ta", "tat", "wz", "wzt", "wy", "wyt", "twz", "twy",
         "collect", "place", "spread", "gather", "order")


def parts(x):
    high = x.astype(BF16)
    low = (x - high.astype(F32)).astype(BF16)
    return high, low


def rows_dot(table, x):
    high, low = parts(x)
    k = x.shape[0]
    return jnp.dot(
        jnp.concatenate([table[:, :k], table[:, :k], table[:, k:]], 1),
        jnp.concatenate([high, low, high], 0),
        preferred_element_type=F32,
    )


def lanes_dot(x, table):
    high, low = parts(x)
    k = x.shape[1]
    return jnp.dot(
        jnp.concatenate([high, low, high], 1),
        jnp.concatenate([table[:k], table[:k], table[k:]], 0),
        preferred_element_type=F32,
    )


def exact_dot(x, y):
    return jnp.dot(x, y, precision=HIGHEST, preferred_element_type=F32)


def turn_by(re, im, cosine, sine):
    return re * cosine - im * sine, re * sine + im * cosine


def turn_back(re, im, cosine, sine):
    return re * cosine + im * sine, im * cosine - re * sine


def times_root(value, k, n, sign):
    re, im = value
    if k == 0:
        return value
    if 4 * k == n:
        return (-im, re) if sign > 0 else (im, -re)
    cosine, sine = math.cos(2.0 * math.pi * k / n), sign * math.sin(2.0 * math.pi * k / n)
    if 8 * k == n:
        return ((re - im) * cosine, (re + im) * cosine) if sign > 0 else ((re + im) * cosine, (im - re) * cosine)
    return re * cosine - im * sine, re * sine + im * cosine


def short_transform(values, sign):
    n = len(values)
    if n == 1:
        return values
    even, odd = short_transform(values[0::2], sign), short_transform(values[1::2], sign)
    turned = [times_root(odd[k], k, n, sign) for k in range(n // 2)]
    return [(even[k][0] + turned[k][0], even[k][1] + turned[k][1]) for k in range(n // 2)] + [
        (even[k][0] - turned[k][0], even[k][1] - turned[k][1]) for k in range(n // 2)
    ]


def rows_of(values):
    return jnp.concatenate(
        [jnp.concatenate([v[0] for v in values], 0), jnp.concatenate([v[1] for v in values], 0)], 1
    )


def twisted(values, twist, turn):
    return values[:1] + [
        turn(v[0], v[1], twist[0, 8 * k : 8 * k + 8], twist[1, 8 * k : 8 * k + 8])
        for k, v in enumerate(values)
        if k
    ]


def tiles_of(both, start, number):
    return [
        (both[8 * k : 8 * k + 8, :128], both[8 * k : 8 * k + 8, 128:]) for k in range(start, start + number)
    ]


def axis_values(length, weight, fraction, indices):
    signed = jnp.where(indices >= length // 2, indices - length, indices).astype(F32)
    return 2.0 * math.pi / length * (signed + weight * fraction)


RATE = dict(A=(0, 2, 1), B=(2, 4, 1), C=(4, 4, 1), Cb=(7, 3, 1), Bb=(8, 2, 1), Ab=(14, 2, 3), R=(19, 2, 3), B2=(24, 2,
    1), C2=(27, 2, 1))
ONCE = dict(cells=0, tables=0, weigh=5, gS=8, gH=10, m=12, mix=17, gJ1=32, gJ2=37, gJ3=34, gP=38)
ORDER = ("R", "gJ2", "gH", "Ab", "weigh", "gJ1", "mix", "Cb", "B", "m", "C", "C2", "A", "cells", "tables", "gP", "gS",
    "Bb", "B2", "gJ3")
CHUNKED = ("B", "C", "Cb", "Bb", "B2", "C2")
MESH_ID = pl.DeviceIdType.MESH


def kernel(bloch_ref, weight_ref, band_hbm, material_hbm, *refs):
    count = len(NAMES)
    table_hbm = refs[:count]
    (out_hbm, corr_ref, proj_ref, coef, band_in, material, cell, xt, image, search, fields,
     s_a, r_a, s_b, r_b, s_c, r_c, s_d, r_d, s_cell, r_cell, s_small, r_one, r_two, first_sum, mixing,
     send_x, recv_x, send_small, recv_small, cell_sem, in_sem, table_sem, out_sem) = refs[count : -count]
    tab = dict(zip(NAMES, refs[-count:]))
    y_me, xh_me, xl_me = (lax.axis_index(a) for a in ("band_0", "band_1", "slab_0"))
    z_me, c_me = lax.axis_index("slab_1"), lax.axis_index("slab_2")
    zb_me = y_me * 2 + xh_me
    p_me = xl_me * 8 + zb_me
    q_me = z_me * 2 + c_me
    x_me = xh_me * 2 + xl_me

    def wide_peer(k):
        y = (y_me + k // 4) % 4
        x = (x_me + k % 4) % 4
        return {"band_0": y, "band_1": x // 2, "slab_0": x % 2}, (x % 2) * 8 + y * 2 + x // 2

    def deep_peer(k):
        z = (z_me + k // 2) % 4
        c = (c_me + k % 2) % 2
        return {"slab_1": z, "slab_2": c}, z * 2 + c

    def slab_peer(k):
        xl = (xl_me + k // 8) % 2
        z = (z_me + k // 2 % 4) % 4
        c = (c_me + k % 2) % 2
        return {"slab_0": xl, "slab_1": z, "slab_2": c}, xl, z * 2 + c

    def band_copy(t):
        return pltpu.make_async_copy(band_hbm.at[t], band_in.at[t], in_sem.at[t])

    def table_copy(k):
        return pltpu.make_async_copy(table_hbm[k], tab[NAMES[k]], table_sem.at[k])

    material_copy = pltpu.make_async_copy(material_hbm, material, cell_sem.at[2])
    band_copy(0).start()
    table_copy(0).start()
    for t in range(1, 8):
        band_copy(t).start()
    for k in range(1, count):
        table_copy(k).start()
    material_copy.start()

    barrier = pltpu.get_barrier_semaphore()
    for k in range(1, 16):
        pl.semaphore_signal(barrier, inc=1, device_id=wide_peer(k)[0], device_id_type=MESH_ID)
    for k in range(1, 8):
        pl.semaphore_signal(barrier, inc=1, device_id=deep_peer(k)[0], device_id_type=MESH_ID)
    for k in range(9, 16):
        pl.semaphore_signal(barrier, inc=1, device_id=slab_peer(k)[0], device_id_type=MESH_ID)

    fraction = (bloch_ref[0].astype(F32) + 1.0) / KPOINTS
    row = lax.broadcasted_iota(jnp.int32, (N, N), 0)
    lane = lax.broadcasted_iota(jnp.int32, (N, N), 1)
    qx = axis_values(N, 0.5, fraction, row)
    qz = axis_values(N, 0.2, fraction, zb_me * 16 + lane // 8)
    qy = axis_values(N, 0.35, fraction, (xl_me * 8 + q_me) * 8 + lane % 8)
    planar = jnp.sqrt(qx * qx + qy * qy)
    magnitude = jnp.sqrt(planar * planar + qz * qz)
    coef[0] = magnitude * (qx * qz / (magnitude * planar))
    coef[1] = magnitude * (qy * qz / (magnitude * planar))
    coef[2] = magnitude * (-planar / magnitude)
    coef[3] = magnitude * (qy / planar)
    coef[4] = magnitude * (-qx / planar)
    coef[5] = 1.0 / (magnitude * magnitude + 1.0)
    pl.semaphore_wait(barrier, 29)
    table_copy(0).wait()

    def send(kind, t, source, target, peers, number, me):
        for k in range(1, number):
            device, slot = peers(k)
            pltpu.make_async_remote_copy(
                src_ref=source.at[slot], dst_ref=target.at[me],
                send_sem=send_x.at[kind, t], recv_sem=recv_x.at[kind, t],
                device_id=device, device_id_type=MESH_ID,
            ).start()
        target[me] = source[me]

    def descriptor(kind, t, source, target, number):
        return pltpu.make_async_remote_copy(
            src_ref=source.at[pl.ds(0, number - 1)], dst_ref=target.at[pl.ds(0, number - 1)],
            send_sem=send_x.at[kind, t], recv_sem=recv_x.at[kind, t],
            device_id=deep_peer(1)[0], device_id_type=MESH_ID,
        )

    def start_sum(slot):
        for k in range(1, 16):
            pltpu.make_async_remote_copy(
                src_ref=s_small.at[slot, 0], dst_ref=r_one.at[slot, p_me],
                send_sem=send_small.at[slot, 0], recv_sem=recv_small.at[slot, 0],
                device_id=wide_peer(k)[0], device_id_type=MESH_ID,
            ).start()
        r_one[slot, p_me] = s_small[slot, 0]

    def small_wait(slot, step, target, number):
        return pltpu.make_async_remote_copy(
            src_ref=target.at[slot, pl.ds(0, number - 1)], dst_ref=target.at[slot, pl.ds(0, number - 1)],
            send_sem=send_small.at[slot, step], recv_sem=recv_small.at[slot, step],
            device_id=deep_peer(1)[0], device_id_type=MESH_ID,
        )

    def middle_sum(slot):
        small_wait(slot, 0, r_one, 16).wait_recv()
        s_small[slot, 1] = jnp.sum(r_one[slot], axis=0)
        for k in range(1, 8):
            pltpu.make_async_remote_copy(
                src_ref=s_small.at[slot, 1], dst_ref=r_two.at[slot, q_me],
                send_sem=send_small.at[slot, 1], recv_sem=recv_small.at[slot, 1],
                device_id=deep_peer(k)[0], device_id_type=MESH_ID,
            ).start()
        r_two[slot, q_me] = s_small[slot, 1]

    def finish_sum(slot):
        small_wait(slot, 1, r_two, 8).wait_recv()
        return jnp.sum(r_two[slot], axis=0)

    def send_materials():
        material_copy.wait()
        for q in range(8):
            s_cell[q] = material[q].astype(F32).T.reshape(16, 8, N)
        me = xl_me * 8 + q_me
        for k in range(1, 16):
            device, xl, q = slab_peer(k)
            pltpu.make_async_remote_copy(
                src_ref=s_cell.at[q, xl * 8 + zb_me], dst_ref=r_cell.at[me],
                send_sem=cell_sem.at[0], recv_sem=cell_sem.at[1],
                device_id=device, device_id_type=MESH_ID,
            ).start()
        r_cell[me] = s_cell[q_me, p_me]

    cell_wait = pltpu.make_async_remote_copy(
        src_ref=r_cell.at[pl.ds(0, 15)], dst_ref=r_cell.at[pl.ds(0, 15)],
        send_sem=cell_sem.at[0], recv_sem=cell_sem.at[1],
        device_id=deep_peer(1)[0], device_id_type=MESH_ID,
    )

    def weigh_cells():
        cell_wait.wait_recv()
        kinds = jnp.dot(r_cell[...].reshape(N, N).astype(BF16), tab["order"][...], preferred_element_type=F32)
        met = (row // 8) == (lane // 8)
        placed = jnp.where(met, kinds, 0.0)
        for d in range(1, 16):
            moved = jnp.where(met, pltpu.roll(kinds, 8 * d, 1), 0.0)
            placed = placed + jnp.concatenate([moved[8 * d :], moved[: 8 * d]], 0)
        weights = jnp.zeros((N, N), F32)
        for kind in range(weight_ref.shape[0]):
            weights = weights + jnp.where(placed == float(kind), weight_ref[kind], 0.0)
        cell[...] = weights / CELLS

    def curl_and_send(kind, t, block):
        columns = []
        for c in range(3):
            halves = []
            for part in range(2):
                term = coef[c] * block[part]
                if c < 2:
                    term = term - coef[3 + c] * block[2 + part]
                halves.append(term)
            columns.append(jnp.concatenate(halves, 0))
        spread_x = rows_dot(tab["ta"], jnp.concatenate(columns, 1))
        op = kind // 4
        for c in range(3):
            s_a[op, 3 * t + c] = spread_x[:, c * N : (c + 1) * N].reshape(16, 2, 8, N)

        def body(c, carry):
            k = 3 * t + c
            send(kind, k, s_a.at[op, k], r_a.at[op, k], wide_peer, 16, p_me)
            return carry

        lax.fori_loop(0, 3, body, 0)

    def z_stage(kind, k):
        op = kind // 4
        descriptor(kind - 1, k, s_a.at[op, k], r_a.at[op, k], 16).wait_recv()
        values = []
        for xlo in range(2):
            arrived = [(r_a[op, k, xlo * 8 + z, 0], r_a[op, k, xlo * 8 + z, 1]) for z in range(8)]
            values += twisted(short_transform(arrived, 1), tab["twz"], turn_by)
        both = lanes_dot(rows_of(values), tab["wz"])
        for xlo in range(2):
            for part in range(2):
                s_b[op, k, :, xlo, part] = both[xlo * 64 : (xlo + 1) * 64, part * N : (part + 1) * N].reshape(8, 8, N)
        send(kind, k, s_b.at[op, k], r_b.at[op, k], deep_peer, 8, q_me)

    def y_stage(kind, k):
        op = kind // 4
        descriptor(kind, k, s_b.at[op, k], r_b.at[op, k], 8).wait_recv()
        arrived = [(r_b[op, k, y % 8, y // 8, 0], r_b[op, k, y % 8, y // 8, 1]) for y in range(16)]
        values = twisted(short_transform(arrived, 1), tab["twy"], turn_by)
        both = lanes_dot(rows_of(values), tab["wy"])
        for part in range(2):
            fields[k // 3, k % 3, part] = both[:, part * N : (part + 1) * N].reshape(16, 8, N)

    def y_back_stage(k):
        weights = cell[...]
        both = jnp.concatenate([fields[k // 3, k % 3, part].reshape(N, N) * weights for part in range(2)], 1)
        mixed = tiles_of(lanes_dot(both, tab["wyt"]), 0, 16)
        for y, (re, im) in enumerate(short_transform(twisted(mixed, tab["twy"], turn_back), -1)):
            s_c[k, y % 8, y // 8, 0] = re
            s_c[k, y % 8, y // 8, 1] = im
        send(2, k, s_c.at[k], r_c.at[k], deep_peer, 8, q_me)

    def z_back_stage(k):
        descriptor(2, k, s_c.at[k], r_c.at[k], 8).wait_recv()
        rows = [
            jnp.concatenate([r_c[k, :, xlo, part].reshape(64, N) for part in range(2)], 1) for xlo in range(2)
        ]
        both = lanes_dot(jnp.concatenate(rows, 0), tab["wzt"])
        for xlo in range(2):
            mixed = twisted(tiles_of(both, xlo * 8, 8), tab["twz"], turn_back)
            for z, (re, im) in enumerate(short_transform(mixed, -1)):
                s_d[k, xlo * 8 + z, 0] = re
                s_d[k, xlo * 8 + z, 1] = im
        send(3, k, s_d.at[k], r_d.at[k], wide_peer, 16, p_me)

    def x_back_stage(t):
        columns = []
        for c in range(3):
            k = 3 * t + c
            descriptor(3, k, s_d.at[k], r_d.at[k], 16).wait_recv()
            columns.append(r_d[k].reshape(256, N))
        back = rows_dot(tab["tat"], jnp.concatenate(columns, 1))
        for part in range(2):
            g = [back[part * N : (part + 1) * N, c * N : (c + 1) * N] for c in range(3)]
            image[t, 0, part] = (g[0] * coef[0] + g[1] * coef[1] + g[2] * coef[2]).reshape(16, 8, N)
            image[t, 1, part] = (-(g[0] * coef[3] + g[1] * coef[4])).reshape(16, 8, N)

    def gram(left, right, groups, slot, scale=None):
        def body(g, total):
            comp, m0 = g // 2, (g % 2) * 8
            left_cols = jnp.concatenate([left[:, comp, :, m0 + m].reshape(N, N) for m in range(8)], 1)
            if scale is None:
                right_cols = left_cols if right is left else jnp.concatenate(
                    [right[:, comp, :, m0 + m].reshape(N, N) for m in range(8)], 1
                )
            else:
                right_cols = []
                for m in range(8):
                    weight = scale[pl.ds(pl.multiple_of((m0 + m) * 8, 8), 8), :]
                    right_cols.append((right[:, comp, :, m0 + m] * weight[None, None]).reshape(N, N))
                right_cols = jnp.concatenate(right_cols, 1)
            lefts = jnp.concatenate(parts(left_cols), 0)
            rights = lefts if right_cols is left_cols else jnp.concatenate(parts(right_cols), 0)
            both = lax.dot_general(lefts, rights, (((1,), (1,)), ((), ())), preferred_element_type=F32)
            return total + (both[:N, :N] + ((both[:N, N:] + both[N:, :N]) + both[N:, N:]))

        total = lax.fori_loop(0, groups, body, jnp.zeros((N, N), F32))
        folded = exact_dot(tab["collect"][...], jnp.where(row % 8 == lane % 8, total, 0.0))
        sums = exact_dot(folded[:8], tab["place"][0]) + exact_dot(folded[8:], tab["place"][1])
        return pltpu.roll(sums, 16 * slot, 1) if slot else sums

    def mix():
        top = finish_sum(0)
        first_sum[...] = top
        left = lax.broadcasted_iota(jnp.int32, (8, N), 1) % 16 < 8
        below = jnp.where(left, -pltpu.roll(top, N - 8, 1), pltpu.roll(top, 8, 1))
        system = jnp.concatenate([top, below], 0)
        rows16 = lax.broadcasted_iota(jnp.int32, (16, N), 0)
        for k in range(16):
            pivot = system[k : k + 1] / system[k : k + 1, k : k + 1]
            system = jnp.where(rows16 == k, pivot, system - system[:, k : k + 1] * pivot)
        wide = exact_dot(system, tab["spread"][...])
        spread_out = jnp.where(row % 8 == lane % 8, exact_dot(tab["gather"][...], wide).T, 0.0)
        mix_high, mix_low = parts(spread_out)
        mixing[:, :N] = mix_high
        mixing[:, N:] = mix_low

        def body(g, carry):
            comp, m0 = g // 2, (g % 2) * 8
            columns = jnp.concatenate([xt[:, comp, :, m0 + m].reshape(N, N) for m in range(8)], 1)
            mixed = rows_dot(mixing, columns)
            for m in range(8):
                search[:, comp, :, m0 + m] = mixed[:, m * N : (m + 1) * N].reshape(8, 2, 8, N)
            return carry

        lax.fori_loop(0, 4, body, 0)

    def out_copy(t):
        return pltpu.make_async_copy(band_in.at[t], out_hbm.at[t], out_sem.at[t])

    def residual(t):
        block = []
        for comp in range(2):
            for part in range(2):
                left = (image[t, comp, part] - search[t, comp, part]).reshape(N, N) * coef[5]
                search[t, comp, part] = left.reshape(16, 8, N)
                block.append(left)
        curl_and_send(4, t, block)
        for comp in range(2):
            for part in range(2):
                band_in[t, comp, part] = block[comp * 2 + part].T.reshape(16, 8, N)
        out_copy(t).start()

    def load(t):
        band_copy(t).wait()
        for comp in range(2):
            for part in range(2):
                xt[t, comp, part] = band_in[t, comp, part].reshape(N, N).T.reshape(16, 8, N)
        curl_and_send(0, t, [xt[t, c, r].reshape(N, N) for c in range(2) for r in range(2)])

    def rest_of_tables():
        for k in range(1, count):
            table_copy(k).wait()

    def overlaps():
        s_small[0, 0] = gram(xt, xt, 4, 0)

    def overlaps_of_image():
        s_small[0, 0] = s_small[0, 0] + gram(fields, fields, 6, 1, cell)
        start_sum(0)

    def first_overlaps_of_search():
        s_small[1, 0] = gram(xt, search, 4, 0)

    def add_overlaps(left, right, groups, slot, scale=None):
        s_small[1, 0] = s_small[1, 0] + gram(left, right, groups, slot, scale)

    stages = dict(
        A=load,
        B=lambda t: z_stage(1, t),
        C=lambda t: y_stage(1, t),
        Cb=y_back_stage,
        Bb=z_back_stage,
        Ab=x_back_stage,
        R=residual,
        B2=lambda t: z_stage(5, t),
        C2=lambda t: y_stage(5, t),
    )
    once = dict(
        cells=send_materials,
        tables=rest_of_tables,
        weigh=weigh_cells,
        gS=overlaps,
        gH=overlaps_of_image,
        m=lambda: middle_sum(0),
        mix=mix,
        gJ1=first_overlaps_of_search,
        gJ2=lambda: add_overlaps(search, search, 4, 1),
        gJ3=lambda: add_overlaps(search, image, 4, 2),
        gP=lambda: add_overlaps(fields, fields, 6, 3, cell),
    )

    def run(t, name):
        if name in ONCE:
            pl.when(t == ONCE[name])(once[name])
            return
        first, count_of, per = RATE[name]
        total = 24 if name in CHUNKED else 8

        def body(k, carry):
            stages[name](k)
            return carry

        @pl.when((t >= first) & (t <= first + (total * per - 1) // count_of))
        def _():
            since = t - first
            lax.fori_loop(since * count_of // per, jnp.minimum((since + 1) * count_of // per, total), body, 0)

    def step(t, carry):
        for name in ORDER:
            run(t, name)
        return carry

    lax.fori_loop(0, ONCE["gP"] + 1, step, 0)

    start_sum(1)
    middle_sum(1)
    second = finish_sum(1) / CELLS
    first = first_sum[...] / CELLS
    flipped = jnp.concatenate([second, jnp.zeros((N - 8, N), F32)], 0).T

    def joined(corner, right, below, last):
        return jnp.concatenate(
            [jnp.concatenate([corner, right], 1), jnp.concatenate([below, last], 1)], 0
        )

    corr_ref[0] = joined(first[:8, 0:8], second[:8, 0:8], flipped[0:8, :8], second[:8, 16:24])
    corr_ref[1] = joined(first[:8, 8:16], second[:8, 8:16], -flipped[8:16, :8], second[:8, 24:32])
    proj_ref[0] = joined(first[:8, 16:24], flipped[32:40, :8], second[:8, 32:40], second[:8, 48:56])
    proj_ref[1] = joined(first[:8, 24:32], -flipped[40:48, :8], second[:8, 40:48], second[:8, 56:64])

    def drain(t, carry):
        descriptor(0, t, s_a.at[0, t], r_a.at[0, t], 16).wait_send()
        descriptor(1, t, s_b.at[0, t], r_b.at[0, t], 8).wait_send()
        descriptor(2, t, s_c.at[t], r_c.at[t], 8).wait_send()
        descriptor(3, t, s_d.at[t], r_d.at[t], 16).wait_send()
        descriptor(4, t, s_a.at[1, t], r_a.at[1, t], 16).wait_send()
        descriptor(5, t, s_b.at[1, t], r_b.at[1, t], 8).wait_send()
        return carry

    lax.fori_loop(0, 24, drain, 0)
    for t in range(8):
        out_copy(t).wait()
    cell_wait.wait_send()
    for slot in range(2):
        small_wait(slot, 0, r_one, 16).wait_send()
        small_wait(slot, 1, r_two, 8).wait_send()


def shards(band_block, material_grid, inverse_permittivity, bloch_index):
    table = {name: jnp.asarray(value) for name, value in tables().items()}
    vmem = pl.BlockSpec(memory_space=pltpu.VMEM)
    smem = pl.BlockSpec(memory_space=pltpu.SMEM)
    anywhere = pl.BlockSpec(memory_space=pl.ANY)
    block = (8, 2, 2, 16, 8, N)
    return pl.pallas_call(
        kernel,
        out_shape=(
            jax.ShapeDtypeStruct(band_block.shape, F32),
            jax.ShapeDtypeStruct((2, 16, 16), F32),
            jax.ShapeDtypeStruct((2, 16, 16), F32),
        ),
        in_specs=[smem, smem] + [anywhere] * (2 + len(NAMES)),
        out_specs=(anywhere, vmem, vmem),
        scratch_shapes=[
            pltpu.VMEM((6, N, N), F32),
            pltpu.VMEM(block, F32),
            pltpu.VMEM((8, N, N), jnp.int32),
            pltpu.VMEM((N, N), F32),
            pltpu.VMEM(block, F32),
            pltpu.VMEM(block, F32),
            pltpu.VMEM(block, F32),
            pltpu.VMEM((8, 3, 2, 16, 8, N), F32),
            pltpu.VMEM((2, 24, 16, 2, 8, N), F32),
            pltpu.VMEM((2, 24, 16, 2, 8, N), F32),
            pltpu.VMEM((2, 24, 8, 2, 2, 8, N), F32),
            pltpu.VMEM((2, 24, 8, 2, 2, 8, N), F32),
            pltpu.VMEM((24, 8, 2, 2, 8, N), F32),
            pltpu.VMEM((24, 8, 2, 2, 8, N), F32),
            pltpu.VMEM((24, 16, 2, 8, N), F32),
            pltpu.VMEM((24, 16, 2, 8, N), F32),
            pltpu.VMEM((8, 16, 8, N), F32),
            pltpu.VMEM((16, 8, N), F32),
            pltpu.VMEM((2, 2, 8, N), F32),
            pltpu.VMEM((2, 16, 8, N), F32),
            pltpu.VMEM((2, 8, 8, N), F32),
            pltpu.VMEM((8, N), F32),
            pltpu.VMEM((N, 2 * N), BF16),
            pltpu.SemaphoreType.DMA((6, 24)),
            pltpu.SemaphoreType.DMA((6, 24)),
            pltpu.SemaphoreType.DMA((2, 2)),
            pltpu.SemaphoreType.DMA((2, 2)),
            pltpu.SemaphoreType.DMA((3,)),
            pltpu.SemaphoreType.DMA((8,)),
            pltpu.SemaphoreType.DMA((len(NAMES),)),
            pltpu.SemaphoreType.DMA((8,)),
        ] + [pltpu.VMEM(table[name].shape, table[name].dtype) for name in NAMES],
        compiler_params=pltpu.CompilerParams(
            collective_id=0, has_side_effects=True, vmem_limit_bytes=63 * 1024 * 1024
        ),
    )(bloch_index, inverse_permittivity, band_block, material_grid, *[table[name] for name in NAMES])


def solution(mesh):
    finer = Mesh(
        mesh.devices.reshape(4, 2, 2, 4, 2), ("band_0", "band_1", "slab_0", "slab_1", "slab_2")
    )
    placed = (P(None, None, None, BAND, SLAB, None), P(SLAB, None, None), P(), P())
    return jax.shard_map(
        shards,
        mesh=finer,
        in_specs=placed,
        out_specs=(P(None, None, None, BAND, SLAB, None), P(), P()),
        check_vma=False,
    )
```

```python
import functools
import math

import jax
import jax.numpy as jnp
import numpy as np
from jax import lax
from jax.experimental import pallas as pl
from jax.experimental.pallas import tpu as pltpu
from jax.sharding import Mesh
from jax.sharding import PartitionSpec as P

KPOINTS = 8
N = 128
CELLS = N * N * N
BANDS = 8
BAND = ("band_0", "band_1")
SLAB = ("slab_0", "slab_1", "slab_2")
HIGHEST = lax.Precision.HIGHEST
F32 = jnp.float32
BF16 = jnp.bfloat16


def _rot(angle):
    c, s = np.cos(angle), np.sin(angle)
    return np.stack([np.stack([c, -s]), np.stack([s, c])])


def _halves(table):
    high = table.astype(BF16)
    low = (table - high.astype(np.float64)).astype(BF16)
    return high, low


def _left(table):
    high, low = _halves(table)
    return np.concatenate([high, low], 1)


def _right(table):
    high, low = _halves(table)
    return np.concatenate([high, low], 0)


def tables():
    tau = 2.0 * math.pi
    i128, i16, i8 = np.arange(128), np.arange(16), np.arange(8)
    r = _rot(tau / 128 * (i128[:, None] * i128[None, :] % 128))
    ta = r.reshape(2, 2, 16, 8, 128).transpose(2, 0, 3, 1, 4).reshape(256, 256)
    r = _rot(tau / 16 * (i16[:, None] * i16[None, :] % 16))
    wz = np.einsum("abos,xy->bsxaoy", r, np.eye(8)).reshape(256, 256)
    r = _rot(tau / 8 * (i8[:, None] * i8[None, :] % 8))
    wy = np.einsum("abos,xy->bxsayo", r, np.eye(16)).reshape(256, 256)
    lane = np.arange(128)
    az = tau / 128 * ((np.arange(64) // 8)[:, None] * (lane // 8)[None, :])
    ay = tau / 128 * ((np.arange(128) // 8)[:, None] * (lane % 8)[None, :])
    twz = np.stack([np.cos(az), np.sin(az)]).astype(np.float32)
    twy = np.stack([np.cos(ay), np.sin(ay)]).astype(np.float32)
    gather = np.zeros((128, 16), np.float32)
    for band in range(8):
        for part in range(2):
            gather[(band * 2 + part) * 8 : (band * 2 + part + 1) * 8, part * 8 + band] = 1.0
    turn = np.zeros((16, 16), np.float32)
    turn[:8, 8:] = np.eye(8)
    turn[8:, :8] = -np.eye(8)
    turned = gather @ turn.T
    collect = np.concatenate([gather.T[:8], turned.T[:8]], 0)
    place = np.zeros((2, 128, 128), np.float32)
    place[0, :, :16] = gather
    place[1, :, :16] = turned
    spread = np.zeros((128, 128), np.float32)
    spread[16:32] = gather.T
    order = np.zeros((128, 128), np.float32)
    order[lane, lane % 16 * 8 + lane // 16] = 1.0
    return dict(
        ta=_left(ta), tat=_left(ta.T),
        wz=_right(wz), wzt=_right(wz.T), wy=_right(wy), wyt=_right(wy.T),
        twz=twz, twy=twy, collect=collect, place=place, spread=spread, gather=gather, order=order.astype(BF16),
    )


NAMES = ("ta", "tat", "wz", "wzt", "wy", "wyt", "twz", "twy",
         "collect", "place", "spread", "gather", "order")


def parts(x):
    high = x.astype(BF16)
    low = (x - high.astype(F32)).astype(BF16)
    return high, low


def rows_dot(table, x):
    high, low = parts(x)
    k = x.shape[0]
    return jnp.dot(
        jnp.concatenate([table[:, :k], table[:, :k], table[:, k:]], 1),
        jnp.concatenate([high, low, high], 0),
        preferred_element_type=F32,
    )


def lanes_dot(x, table):
    high, low = parts(x)
    k = x.shape[1]
    return jnp.dot(
        jnp.concatenate([high, low, high], 1),
        jnp.concatenate([table[:k], table[:k], table[k:]], 0),
        preferred_element_type=F32,
    )


def exact_dot(x, y):
    return jnp.dot(x, y, precision=HIGHEST, preferred_element_type=F32)


def turn_by(re, im, cosine, sine):
    return re * cosine - im * sine, re * sine + im * cosine


def turn_back(re, im, cosine, sine):
    return re * cosine + im * sine, im * cosine - re * sine


def times_root(value, k, n, sign):
    re, im = value
    if k == 0:
        return value
    if 4 * k == n:
        return (-im, re) if sign > 0 else (im, -re)
    cosine, sine = math.cos(2.0 * math.pi * k / n), sign * math.sin(2.0 * math.pi * k / n)
    if 8 * k == n:
        return ((re - im) * cosine, (re + im) * cosine) if sign > 0 else ((re + im) * cosine, (im - re) * cosine)
    return re * cosine - im * sine, re * sine + im * cosine


def short_transform(values, sign):
    n = len(values)
    if n == 1:
        return values
    even, odd = short_transform(values[0::2], sign), short_transform(values[1::2], sign)
    turned = [times_root(odd[k], k, n, sign) for k in range(n // 2)]
    return [(even[k][0] + turned[k][0], even[k][1] + turned[k][1]) for k in range(n // 2)] + [
        (even[k][0] - turned[k][0], even[k][1] - turned[k][1]) for k in range(n // 2)
    ]


def rows_of(values):
    return jnp.concatenate(
        [jnp.concatenate([v[0] for v in values], 0), jnp.concatenate([v[1] for v in values], 0)], 1
    )


def twisted(values, twist, turn):
    return values[:1] + [
        turn(v[0], v[1], twist[0, 8 * k : 8 * k + 8], twist[1, 8 * k : 8 * k + 8])
        for k, v in enumerate(values)
        if k
    ]


def tiles_of(both, start, number):
    return [
        (both[8 * k : 8 * k + 8, :128], both[8 * k : 8 * k + 8, 128:]) for k in range(start, start + number)
    ]


def axis_values(length, weight, fraction, indices):
    signed = jnp.where(indices >= length // 2, indices - length, indices).astype(F32)
    return 2.0 * math.pi / length * (signed + weight * fraction)


RATE = dict(A=(0, 2, 1), B=(2, 4, 1), C=(4, 4, 1), Cb=(7, 3, 1), Bb=(8, 2, 1), Ab=(14, 2, 3), R=(19, 2, 3), B2=(24, 2,
    1), C2=(27, 2, 1))
ONCE = dict(cells=0, tables=0, weigh=5, gS=8, gH=10, m=12, mix=17, gJ1=32, gJ2=37, gJ3=34, gP=38)
ORDER = ("R", "gJ2", "gH", "Ab", "weigh", "gJ1", "mix", "Cb", "B", "m", "C", "C2", "A", "cells", "tables", "gP", "gS",
    "Bb", "B2", "gJ3")
CHUNKED = ("B", "C", "Cb", "Bb", "B2", "C2")
MESH_ID = pl.DeviceIdType.MESH


def kernel(bloch_ref, weight_ref, band_hbm, material_hbm, *refs):
    count = len(NAMES)
    table_hbm = refs[:count]
    (out_ref, corr_ref, proj_ref, coef, band_in, material, cell, xt, image, search, fields,
     s_a, r_a, s_b, r_b, s_c, r_c, s_d, r_d, s_cell, r_cell, s_small, r_one, r_two, first_sum, mixing,
     send_x, recv_x, send_small, recv_small, cell_sem, in_sem, table_sem) = refs[count : -count]
    tab = dict(zip(NAMES, refs[-count:]))
    y_me, xh_me, xl_me = (lax.axis_index(a) for a in ("band_0", "band_1", "slab_0"))
    z_me, c_me = lax.axis_index("slab_1"), lax.axis_index("slab_2")
    zb_me = y_me * 2 + xh_me
    p_me = xl_me * 8 + zb_me
    q_me = z_me * 2 + c_me
    x_me = xh_me * 2 + xl_me

    def wide_peer(k):
        y = (y_me + k // 4) % 4
        x = (x_me + k % 4) % 4
        return {"band_0": y, "band_1": x // 2, "slab_0": x % 2}, (x % 2) * 8 + y * 2 + x // 2

    def deep_peer(k):
        z = (z_me + k // 2) % 4
        c = (c_me + k % 2) % 2
        return {"slab_1": z, "slab_2": c}, z * 2 + c

    def slab_peer(k):
        xl = (xl_me + k // 8) % 2
        z = (z_me + k // 2 % 4) % 4
        c = (c_me + k % 2) % 2
        return {"slab_0": xl, "slab_1": z, "slab_2": c}, xl, z * 2 + c

    def band_copy(t):
        return pltpu.make_async_copy(band_hbm.at[t], band_in.at[t], in_sem.at[t])

    def table_copy(k):
        return pltpu.make_async_copy(table_hbm[k], tab[NAMES[k]], table_sem.at[k])

    material_copy = pltpu.make_async_copy(material_hbm, material, cell_sem.at[2])
    band_copy(0).start()
    table_copy(0).start()
    for t in range(1, 8):
        band_copy(t).start()
    for k in range(1, count):
        table_copy(k).start()
    material_copy.start()

    barrier = pltpu.get_barrier_semaphore()
    for k in range(1, 16):
        pl.semaphore_signal(barrier, inc=1, device_id=wide_peer(k)[0], device_id_type=MESH_ID)
    for k in range(1, 8):
        pl.semaphore_signal(barrier, inc=1, device_id=deep_peer(k)[0], device_id_type=MESH_ID)
    for k in range(9, 16):
        pl.semaphore_signal(barrier, inc=1, device_id=slab_peer(k)[0], device_id_type=MESH_ID)

    fraction = (bloch_ref[0].astype(F32) + 1.0) / KPOINTS
    row = lax.broadcasted_iota(jnp.int32, (N, N), 0)
    lane = lax.broadcasted_iota(jnp.int32, (N, N), 1)
    qx = axis_values(N, 0.5, fraction, row)
    qz = axis_values(N, 0.2, fraction, zb_me * 16 + lane // 8)
    qy = axis_values(N, 0.35, fraction, (xl_me * 8 + q_me) * 8 + lane % 8)
    planar = jnp.sqrt(qx * qx + qy * qy)
    magnitude = jnp.sqrt(planar * planar + qz * qz)
    coef[0] = magnitude * (qx * qz / (magnitude * planar))
    coef[1] = magnitude * (qy * qz / (magnitude * planar))
    coef[2] = magnitude * (-planar / magnitude)
    coef[3] = magnitude * (qy / planar)
    coef[4] = magnitude * (-qx / planar)
    coef[5] = 1.0 / (magnitude * magnitude + 1.0)
    pl.semaphore_wait(barrier, 29)
    table_copy(0).wait()

    def send(kind, t, source, target, peers, number, me):
        for k in range(1, number):
            device, slot = peers(k)
            pltpu.make_async_remote_copy(
                src_ref=source.at[slot], dst_ref=target.at[me],
                send_sem=send_x.at[kind, t], recv_sem=recv_x.at[kind, t],
                device_id=device, device_id_type=MESH_ID,
            ).start()
        target[me] = source[me]

    def descriptor(kind, t, source, target, number):
        return pltpu.make_async_remote_copy(
            src_ref=source.at[pl.ds(0, number - 1)], dst_ref=target.at[pl.ds(0, number - 1)],
            send_sem=send_x.at[kind, t], recv_sem=recv_x.at[kind, t],
            device_id=deep_peer(1)[0], device_id_type=MESH_ID,
        )

    def start_sum(slot):
        for k in range(1, 16):
            pltpu.make_async_remote_copy(
                src_ref=s_small.at[slot, 0], dst_ref=r_one.at[slot, p_me],
                send_sem=send_small.at[slot, 0], recv_sem=recv_small.at[slot, 0],
                device_id=wide_peer(k)[0], device_id_type=MESH_ID,
            ).start()
        r_one[slot, p_me] = s_small[slot, 0]

    def small_wait(slot, step, target, number):
        return pltpu.make_async_remote_copy(
            src_ref=target.at[slot, pl.ds(0, number - 1)], dst_ref=target.at[slot, pl.ds(0, number - 1)],
            send_sem=send_small.at[slot, step], recv_sem=recv_small.at[slot, step],
            device_id=deep_peer(1)[0], device_id_type=MESH_ID,
        )

    def middle_sum(slot):
        small_wait(slot, 0, r_one, 16).wait_recv()
        s_small[slot, 1] = jnp.sum(r_one[slot], axis=0)
        for k in range(1, 8):
            pltpu.make_async_remote_copy(
                src_ref=s_small.at[slot, 1], dst_ref=r_two.at[slot, q_me],
                send_sem=send_small.at[slot, 1], recv_sem=recv_small.at[slot, 1],
                device_id=deep_peer(k)[0], device_id_type=MESH_ID,
            ).start()
        r_two[slot, q_me] = s_small[slot, 1]

    def finish_sum(slot):
        small_wait(slot, 1, r_two, 8).wait_recv()
        return jnp.sum(r_two[slot], axis=0)

    def send_materials():
        material_copy.wait()
        for q in range(8):
            s_cell[q] = material[q].astype(F32).T.reshape(16, 8, N)
        me = xl_me * 8 + q_me
        for k in range(1, 16):
            device, xl, q = slab_peer(k)
            pltpu.make_async_remote_copy(
                src_ref=s_cell.at[q, xl * 8 + zb_me], dst_ref=r_cell.at[me],
                send_sem=cell_sem.at[0], recv_sem=cell_sem.at[1],
                device_id=device, device_id_type=MESH_ID,
            ).start()
        r_cell[me] = s_cell[q_me, p_me]

    cell_wait = pltpu.make_async_remote_copy(
        src_ref=r_cell.at[pl.ds(0, 15)], dst_ref=r_cell.at[pl.ds(0, 15)],
        send_sem=cell_sem.at[0], recv_sem=cell_sem.at[1],
        device_id=deep_peer(1)[0], device_id_type=MESH_ID,
    )

    def weigh_cells():
        cell_wait.wait_recv()
        kinds = jnp.dot(r_cell[...].reshape(N, N).astype(BF16), tab["order"][...], preferred_element_type=F32)
        met = (row // 8) == (lane // 8)
        placed = jnp.where(met, kinds, 0.0)
        for d in range(1, 16):
            moved = jnp.where(met, pltpu.roll(kinds, 8 * d, 1), 0.0)
            placed = placed + jnp.concatenate([moved[8 * d :], moved[: 8 * d]], 0)
        weights = jnp.zeros((N, N), F32)
        for kind in range(weight_ref.shape[0]):
            weights = weights + jnp.where(placed == float(kind), weight_ref[kind], 0.0)
        cell[...] = weights / CELLS

    def curl_and_send(kind, t, block):
        columns = []
        for c in range(3):
            halves = []
            for part in range(2):
                term = coef[c] * block[part]
                if c < 2:
                    term = term - coef[3 + c] * block[2 + part]
                halves.append(term)
            columns.append(jnp.concatenate(halves, 0))
        spread_x = rows_dot(tab["ta"], jnp.concatenate(columns, 1))
        op = kind // 4
        for c in range(3):
            s_a[op, 3 * t + c] = spread_x[:, c * N : (c + 1) * N].reshape(16, 2, 8, N)

        def body(c, carry):
            k = 3 * t + c
            send(kind, k, s_a.at[op, k], r_a.at[op, k], wide_peer, 16, p_me)
            return carry

        lax.fori_loop(0, 3, body, 0)

    def z_stage(kind, k):
        op = kind // 4
        descriptor(kind - 1, k, s_a.at[op, k], r_a.at[op, k], 16).wait_recv()
        values = []
        for xlo in range(2):
            arrived = [(r_a[op, k, xlo * 8 + z, 0], r_a[op, k, xlo * 8 + z, 1]) for z in range(8)]
            values += twisted(short_transform(arrived, 1), tab["twz"], turn_by)
        both = lanes_dot(rows_of(values), tab["wz"])
        for xlo in range(2):
            for part in range(2):
                s_b[op, k, :, xlo, part] = both[xlo * 64 : (xlo + 1) * 64, part * N : (part + 1) * N].reshape(8, 8, N)
        send(kind, k, s_b.at[op, k], r_b.at[op, k], deep_peer, 8, q_me)

    def y_stage(kind, k):
        op = kind // 4
        descriptor(kind, k, s_b.at[op, k], r_b.at[op, k], 8).wait_recv()
        arrived = [(r_b[op, k, y % 8, y // 8, 0], r_b[op, k, y % 8, y // 8, 1]) for y in range(16)]
        values = twisted(short_transform(arrived, 1), tab["twy"], turn_by)
        both = lanes_dot(rows_of(values), tab["wy"])
        for part in range(2):
            fields[k // 3, k % 3, part] = both[:, part * N : (part + 1) * N].reshape(16, 8, N)

    def y_back_stage(k):
        weights = cell[...]
        both = jnp.concatenate([fields[k // 3, k % 3, part].reshape(N, N) * weights for part in range(2)], 1)
        mixed = tiles_of(lanes_dot(both, tab["wyt"]), 0, 16)
        for y, (re, im) in enumerate(short_transform(twisted(mixed, tab["twy"], turn_back), -1)):
            s_c[k, y % 8, y // 8, 0] = re
            s_c[k, y % 8, y // 8, 1] = im
        send(2, k, s_c.at[k], r_c.at[k], deep_peer, 8, q_me)

    def z_back_stage(k):
        descriptor(2, k, s_c.at[k], r_c.at[k], 8).wait_recv()
        rows = [
            jnp.concatenate([r_c[k, :, xlo, part].reshape(64, N) for part in range(2)], 1) for xlo in range(2)
        ]
        both = lanes_dot(jnp.concatenate(rows, 0), tab["wzt"])
        for xlo in range(2):
            mixed = twisted(tiles_of(both, xlo * 8, 8), tab["twz"], turn_back)
            for z, (re, im) in enumerate(short_transform(mixed, -1)):
                s_d[k, xlo * 8 + z, 0] = re
                s_d[k, xlo * 8 + z, 1] = im
        send(3, k, s_d.at[k], r_d.at[k], wide_peer, 16, p_me)

    def x_back_stage(t):
        columns = []
        for c in range(3):
            k = 3 * t + c
            descriptor(3, k, s_d.at[k], r_d.at[k], 16).wait_recv()
            columns.append(r_d[k].reshape(256, N))
        back = rows_dot(tab["tat"], jnp.concatenate(columns, 1))
        for part in range(2):
            g = [back[part * N : (part + 1) * N, c * N : (c + 1) * N] for c in range(3)]
            image[t, 0, part] = (g[0] * coef[0] + g[1] * coef[1] + g[2] * coef[2]).reshape(16, 8, N)
            image[t, 1, part] = (-(g[0] * coef[3] + g[1] * coef[4])).reshape(16, 8, N)

    def gram(left, right, groups, slot, scale=None):
        def body(g, total):
            comp, m0 = g // 2, (g % 2) * 8
            left_cols = jnp.concatenate([left[:, comp, :, m0 + m].reshape(N, N) for m in range(8)], 1)
            if scale is None:
                right_cols = left_cols if right is left else jnp.concatenate(
                    [right[:, comp, :, m0 + m].reshape(N, N) for m in range(8)], 1
                )
            else:
                right_cols = []
                for m in range(8):
                    weight = scale[pl.ds(pl.multiple_of((m0 + m) * 8, 8), 8), :]
                    right_cols.append((right[:, comp, :, m0 + m] * weight[None, None]).reshape(N, N))
                right_cols = jnp.concatenate(right_cols, 1)
            lefts = jnp.concatenate(parts(left_cols), 0)
            rights = lefts if right_cols is left_cols else jnp.concatenate(parts(right_cols), 0)
            both = lax.dot_general(lefts, rights, (((1,), (1,)), ((), ())), preferred_element_type=F32)
            return total + (both[:N, :N] + ((both[:N, N:] + both[N:, :N]) + both[N:, N:]))

        total = lax.fori_loop(0, groups, body, jnp.zeros((N, N), F32))
        folded = exact_dot(tab["collect"][...], jnp.where(row % 8 == lane % 8, total, 0.0))
        sums = exact_dot(folded[:8], tab["place"][0]) + exact_dot(folded[8:], tab["place"][1])
        return pltpu.roll(sums, 16 * slot, 1) if slot else sums

    def mix():
        top = finish_sum(0)
        first_sum[...] = top
        left = lax.broadcasted_iota(jnp.int32, (8, N), 1) % 16 < 8
        below = jnp.where(left, -pltpu.roll(top, N - 8, 1), pltpu.roll(top, 8, 1))
        system = jnp.concatenate([top, below], 0)
        rows16 = lax.broadcasted_iota(jnp.int32, (16, N), 0)
        for k in range(16):
            pivot = system[k : k + 1] / system[k : k + 1, k : k + 1]
            system = jnp.where(rows16 == k, pivot, system - system[:, k : k + 1] * pivot)
        wide = exact_dot(system, tab["spread"][...])
        spread_out = jnp.where(row % 8 == lane % 8, exact_dot(tab["gather"][...], wide).T, 0.0)
        mix_high, mix_low = parts(spread_out)
        mixing[:, :N] = mix_high
        mixing[:, N:] = mix_low

        def body(g, carry):
            comp, m0 = g // 2, (g % 2) * 8
            columns = jnp.concatenate([xt[:, comp, :, m0 + m].reshape(N, N) for m in range(8)], 1)
            mixed = rows_dot(mixing, columns)
            for m in range(8):
                search[:, comp, :, m0 + m] = mixed[:, m * N : (m + 1) * N].reshape(8, 2, 8, N)
            return carry

        lax.fori_loop(0, 4, body, 0)

    def residual(t):
        block = []
        for comp in range(2):
            for part in range(2):
                left = (image[t, comp, part] - search[t, comp, part]).reshape(N, N) * coef[5]
                search[t, comp, part] = left.reshape(16, 8, N)
                block.append(left)
        curl_and_send(4, t, block)
        for comp in range(2):
            for part in range(2):
                out_ref[t, comp, part] = block[comp * 2 + part].T.reshape(16, 8, N)

    def load(t):
        band_copy(t).wait()
        for comp in range(2):
            for part in range(2):
                xt[t, comp, part] = band_in[t, comp, part].reshape(N, N).T.reshape(16, 8, N)
        curl_and_send(0, t, [xt[t, c, r].reshape(N, N) for c in range(2) for r in range(2)])

    def rest_of_tables():
        for k in range(1, count):
            table_copy(k).wait()

    def overlaps():
        s_small[0, 0] = gram(xt, xt, 4, 0)

    def overlaps_of_image():
        s_small[0, 0] = s_small[0, 0] + gram(fields, fields, 6, 1, cell)
        start_sum(0)

    def first_overlaps_of_search():
        s_small[1, 0] = gram(xt, search, 4, 0)

    def add_overlaps(left, right, groups, slot, scale=None):
        s_small[1, 0] = s_small[1, 0] + gram(left, right, groups, slot, scale)

    stages = dict(
        A=load,
        B=lambda t: z_stage(1, t),
        C=lambda t: y_stage(1, t),
        Cb=y_back_stage,
        Bb=z_back_stage,
        Ab=x_back_stage,
        R=residual,
        B2=lambda t: z_stage(5, t),
        C2=lambda t: y_stage(5, t),
    )
    once = dict(
        cells=send_materials,
        tables=rest_of_tables,
        weigh=weigh_cells,
        gS=overlaps,
        gH=overlaps_of_image,
        m=lambda: middle_sum(0),
        mix=mix,
        gJ1=first_overlaps_of_search,
        gJ2=lambda: add_overlaps(search, search, 4, 1),
        gJ3=lambda: add_overlaps(search, image, 4, 2),
        gP=lambda: add_overlaps(fields, fields, 6, 3, cell),
    )

    def run(t, name):
        if name in ONCE:
            pl.when(t == ONCE[name])(once[name])
            return
        first, count_of, per = RATE[name]
        total = 24 if name in CHUNKED else 8

        def body(k, carry):
            stages[name](k)
            return carry

        @pl.when((t >= first) & (t <= first + (total * per - 1) // count_of))
        def _():
            since = t - first
            lax.fori_loop(since * count_of // per, jnp.minimum((since + 1) * count_of // per, total), body, 0)

    def step(t, carry):
        for name in ORDER:
            run(t, name)
        return carry

    lax.fori_loop(0, ONCE["gP"] + 1, step, 0)

    start_sum(1)
    middle_sum(1)
    second = finish_sum(1) / CELLS
    first = first_sum[...] / CELLS
    flipped = jnp.concatenate([second, jnp.zeros((N - 8, N), F32)], 0).T

    def joined(corner, right, below, last):
        return jnp.concatenate(
            [jnp.concatenate([corner, right], 1), jnp.concatenate([below, last], 1)], 0
        )

    corr_ref[0] = joined(first[:8, 0:8], second[:8, 0:8], flipped[0:8, :8], second[:8, 16:24])
    corr_ref[1] = joined(first[:8, 8:16], second[:8, 8:16], -flipped[8:16, :8], second[:8, 24:32])
    proj_ref[0] = joined(first[:8, 16:24], flipped[32:40, :8], second[:8, 32:40], second[:8, 48:56])
    proj_ref[1] = joined(first[:8, 24:32], -flipped[40:48, :8], second[:8, 40:48], second[:8, 56:64])

    def drain(t, carry):
        descriptor(0, t, s_a.at[0, t], r_a.at[0, t], 16).wait_send()
        descriptor(1, t, s_b.at[0, t], r_b.at[0, t], 8).wait_send()
        descriptor(2, t, s_c.at[t], r_c.at[t], 8).wait_send()
        descriptor(3, t, s_d.at[t], r_d.at[t], 16).wait_send()
        descriptor(4, t, s_a.at[1, t], r_a.at[1, t], 16).wait_send()
        descriptor(5, t, s_b.at[1, t], r_b.at[1, t], 8).wait_send()
        return carry

    lax.fori_loop(0, 24, drain, 0)
    cell_wait.wait_send()
    for slot in range(2):
        small_wait(slot, 0, r_one, 16).wait_send()
        small_wait(slot, 1, r_two, 8).wait_send()


def shards(band_block, material_grid, inverse_permittivity, bloch_index):
    table = {name: jnp.asarray(value) for name, value in tables().items()}
    vmem = pl.BlockSpec(memory_space=pltpu.VMEM)
    smem = pl.BlockSpec(memory_space=pltpu.SMEM)
    anywhere = pl.BlockSpec(memory_space=pl.ANY)
    block = (8, 2, 2, 16, 8, N)
    return pl.pallas_call(
        kernel,
        out_shape=(
            pltpu.VMEM(band_block.shape, F32),
            pltpu.VMEM((2, 16, 16), F32),
            pltpu.VMEM((2, 16, 16), F32),
        ),
        in_specs=[smem, smem] + [anywhere] * (2 + len(NAMES)),
        out_specs=(vmem, vmem, vmem),
        scratch_shapes=[
            pltpu.VMEM((6, N, N), F32),
            pltpu.VMEM(block, F32),
            pltpu.VMEM((8, N, N), jnp.int32),
            pltpu.VMEM((N, N), F32),
            pltpu.VMEM(block, F32),
            pltpu.VMEM(block, F32),
            pltpu.VMEM(block, F32),
            pltpu.VMEM((8, 3, 2, 16, 8, N), F32),
            pltpu.VMEM((2, 24, 16, 2, 8, N), F32),
            pltpu.VMEM((2, 24, 16, 2, 8, N), F32),
            pltpu.VMEM((2, 24, 8, 2, 2, 8, N), F32),
            pltpu.VMEM((2, 24, 8, 2, 2, 8, N), F32),
            pltpu.VMEM((24, 8, 2, 2, 8, N), F32),
            pltpu.VMEM((24, 8, 2, 2, 8, N), F32),
            pltpu.VMEM((24, 16, 2, 8, N), F32),
            pltpu.VMEM((24, 16, 2, 8, N), F32),
            pltpu.VMEM((8, 16, 8, N), F32),
            pltpu.VMEM((16, 8, N), F32),
            pltpu.VMEM((2, 2, 8, N), F32),
            pltpu.VMEM((2, 16, 8, N), F32),
            pltpu.VMEM((2, 8, 8, N), F32),
            pltpu.VMEM((8, N), F32),
            pltpu.VMEM((N, 2 * N), BF16),
            pltpu.SemaphoreType.DMA((6, 24)),
            pltpu.SemaphoreType.DMA((6, 24)),
            pltpu.SemaphoreType.DMA((2, 2)),
            pltpu.SemaphoreType.DMA((2, 2)),
            pltpu.SemaphoreType.DMA((3,)),
            pltpu.SemaphoreType.DMA((8,)),
            pltpu.SemaphoreType.DMA((len(NAMES),)),
        ] + [pltpu.VMEM(table[name].shape, table[name].dtype) for name in NAMES],
        compiler_params=pltpu.CompilerParams(
            collective_id=0, has_side_effects=True, vmem_limit_bytes=58 * 1024 * 1024
        ),
    )(bloch_index, inverse_permittivity, band_block, material_grid, *[table[name] for name in NAMES])


def solution(mesh):
    finer = Mesh(
        mesh.devices.reshape(4, 2, 2, 4, 2), ("band_0", "band_1", "slab_0", "slab_1", "slab_2")
    )
    placed = (P(None, None, None, BAND, SLAB, None), P(SLAB, None, None), P(), P())
    return jax.shard_map(
        shards,
        mesh=finer,
        in_specs=placed,
        out_specs=(P(None, None, None, BAND, SLAB, None), P(), P()),
        check_vma=False,
    )
```
